256 devices in a mesh: row: 16 (over x, y), col: 16 (over z, core).
Axes of the slice: x: 4, y: 4, z: 8, core: 2. Of those that a mesh axis runs over, the one named last changes fastest.
Arguments:
- values: bfloat16 [8192, 8192], P('row', 'col'), may hold values from 0.0001296997 to 0.12988281
- tile_mask: int32 [64, 64], P('row', 'col'), may hold values 0 or 1
- keep_mask: int32 [64, 64], P('row', 'col'), may hold values 0 or 1
- thr_index: int32 [8192], P('col'), may hold values from 0 to 9
Outputs:
- expanded: bfloat16 [8192, 8192], P('row', 'col')
The draws below stay inside these ranges and needn't reach their ends.
All inputs are finite; a program needn't handle non-finite values. No bound on the sum of `tile_mask` or of `keep_mask` on one device may be relied on, other than what follows from the above.
Results may differ from the reference program's by a relative error of at most 0.0004.
Values may be sent and summed in bfloat16 or wider, within the bound.
A program may use at most 64 MiB of HBM per device.

```python
import math
import jax
import jax.numpy as jnp

TB = 128
NT = 64
ORDER = 8192


def touch_ends(values, stream_key, smallest, largest):
    spot = [jax.random.randint(jax.random.fold_in(stream_key, axis), (), 0, length) for axis, length in enumerate(values.shape)]
    longest = values.shape.index(max(values.shape))
    neighbour = spot[:longest] + [(spot[longest] + 1) % values.shape[longest]] + spot[longest + 1:]
    return values.at[tuple(spot)].set(smallest).at[tuple(neighbour)].set(largest)


def levels(stream_key, extent, shards, least, largest):
    level = 1.0
    for dim, shards_of in shards:
        draws = jax.random.uniform(jax.random.fold_in(jax.random.fold_in(stream_key, 6), dim), (shards_of,), jnp.float32, least / len(shards), largest / len(shards))
        level = level * jnp.repeat(jnp.exp(draws), extent[dim] // shards_of).reshape((-1,) + (1,) * (len(extent) - 1 - dim))
    return level


def setup_inputs(seed: int = 0) -> dict:
    seeds = jax.random.split(jax.random.key(seed), 5)
    values = jnp.clip(jnp.exp(math.log(0.12988281) - 6.909166 * jax.random.uniform(seeds[0], (ORDER, ORDER), jnp.float32) ** levels(seeds[0], (ORDER, ORDER), ((0, 16), (1, 16)), -0.2, 0.2)), 0.0001296997, 0.12988281).astype(jnp.bfloat16)
    tile_mask = touch_ends((jax.random.randint(seeds[1], (NT, NT), 0, 2) < 1).astype(jnp.int32), jax.random.fold_in(seeds[1], 1), 0, 1)
    keep_mask = touch_ends((jax.random.randint(seeds[2], (NT, NT), 0, 4) < 3).astype(jnp.int32), jax.random.fold_in(seeds[2], 1), 0, 1)
    thr_index = touch_ends(jax.random.randint(seeds[3], (ORDER,), 0, 10), jax.random.fold_in(seeds[3], 1), 0, 9).astype(jnp.int32)
    return {"values": values, "tile_mask": tile_mask, "keep_mask": keep_mask, "thr_index": thr_index}


def reference(values, tile_mask, keep_mask, thr_index):
    matrix = (values.reshape(NT, TB, NT, TB) * tile_mask[:, None, :, None].astype(jnp.bfloat16)).reshape(ORDER, ORDER)
    product = jnp.dot(matrix, matrix, preferred_element_type=jnp.float32)
    col_means = jnp.sum(product, axis=0) / ORDER
    thresholds = 0.125 * thr_index.astype(jnp.float32)
    kept_cells = jnp.broadcast_to(keep_mask[:, None, :, None].astype(jnp.float32), (NT, TB, NT, TB)).reshape(ORDER, ORDER)
    pruned = jnp.maximum(product - thresholds * col_means, 0.0) * kept_cells
    col_totals = jnp.sum(pruned, axis=0) / ORDER
    return (pruned / jnp.maximum(col_totals, 0.1)).astype(jnp.bfloat16)
```

```python
import functools

import jax
import jax.numpy as jnp
from jax import lax
from jax.experimental import pallas as pl
from jax.experimental.pallas import tpu as pltpu
from jax.sharding import PartitionSpec as P

TB = 128
BLOCK = 512
HALF = BLOCK // 2
QUART = BLOCK // 4
TILES = BLOCK // TB
GROUP = 16
SIDE = 4
DEPTH = 8
ORDER = BLOCK * GROUP
AUG = 16
EVENTS = 13
MESH = pl.DeviceIdType.MESH

UPPER, LOWER = (0, HALF), (HALF, HALF)


def quarter(half, step):
    return (half[0] + (0 if step > 0 else QUART), QUART)


def plane_queue(axis, step):
    def at(along, across):
        return (along, across) if axis == 0 else (across, along)

    first, second = (UPPER, LOWER) if axis == 0 else (LOWER, UPPER)
    return [
        (at(0, 0), first, 0),
        (at(0, 0), second, 0),
        (at(-step, 0), quarter(first, step), 1),
        (at(0, -1), second, 1),
        (at(0, 1), second, 1),
        (at(-step, 0), quarter(second, step), 2),
        (at(0, 2), second, 3),
        (at(-step, -1), quarter(second, step), 5),
        (at(-step, 1), quarter(second, step), 7),
        (at(-step, 2), quarter(second, step), 9),
    ]


PLANE_ARRIVAL = [1, 2, 3, 5, 7, 8, 9, 10, 11, 12]


def depth_queue(step):
    first, second = (UPPER, LOWER) if step > 0 else (LOWER, UPPER)
    return [
        (0, first, 0),
        (0, second, 0),
        (-step, first, 1),
        (-step, second, 2),
        (-2 * step, first, 4),
        (-2 * step, second, 6),
        (-3 * step, first, 8),
    ]


DEPTH_ARRIVAL = [1, 2, 4, 6, 8, 9, 11]


def wrap(value, size):
    return lax.rem(value + size, size)


def kernel(
    values_ref, tile_hbm, keep_hbm, thr_hbm, pruned_ref, total_ref, tile_ref, keep_ref, thr_ref,
    rows_buf, cols_buf, acc, own, part_buf, sum_buf, tot_buf,
    in_sem, send_sem, recv_sem, part_send, part_recv, sum_send, sum_recv, tot_send, tot_recv,
):
    me_row, me_col = lax.axis_index("row"), lax.axis_index("col")
    x, y = lax.div(me_row, SIDE), lax.rem(me_row, SIDE)
    z, core = lax.div(me_col, 2), lax.rem(me_col, 2)

    def row_of(dx, dy):
        return wrap(x + dx, SIDE) * SIDE + wrap(y + dy, SIDE)

    def col_of(dz, other=0):
        return wrap(z + dz, DEPTH) * 2 + (1 - core if other else core)

    barrier = pltpu.get_barrier_semaphore()

    def greet(i, carry):
        pl.semaphore_signal(barrier, inc=1, device_id=(lax.rem(me_row + i, GROUP), me_col), device_id_type=MESH)
        pl.semaphore_signal(barrier, inc=1, device_id=(me_row, lax.rem(me_col + i, GROUP)), device_id_type=MESH)
        return carry

    lax.fori_loop(1, GROUP, greet, 0)
    loads = [
        pltpu.make_async_copy(out, into, in_sem.at[i])
        for i, (out, into) in enumerate(
            ((values_ref, own), (tile_hbm, tile_ref), (keep_hbm, keep_ref), (thr_hbm, thr_ref))
        )
    ]
    for load in loads:
        load.start()

    copies = []

    def copy_of(buf, slot, rows, number, target):
        part = buf.at[slot, pl.ds(*rows), :]
        return pltpu.make_async_remote_copy(
            src_ref=part, dst_ref=part, send_sem=send_sem.at[number], recv_sem=recv_sem.at[number],
            device_id=target, device_id_type=MESH,
        )

    def add(buf, sent_slot, got_slot, rows, target, leaves, arrives):
        number = len(copies)
        copies.append((
            leaves, arrives,
            copy_of(buf, sent_slot, rows, number, target),
            copy_of(buf, got_slot, rows, number, target),
        ))

    for place in range(10):
        for axis in (0, 1):
            for step in (1, -1):
                (dx, dy), rows, leaves = plane_queue(axis, step)[place]
                sx, sy = (step, 0) if axis == 0 else (0, step)
                add(
                    cols_buf, row_of(dx, dy), row_of(dx - sx, dy - sy), rows,
                    (row_of(sx, sy), me_col), leaves, PLANE_ARRIVAL[place],
                )
        if place < 7:
            for step in (1, -1):
                dz, rows, leaves = depth_queue(step)[place]
                add(
                    rows_buf, col_of(dz), col_of(dz - step), rows,
                    (me_row, col_of(step)), leaves, DEPTH_ARRIVAL[place],
                )
    partner = (me_row, col_of(0, 1))
    for half in (UPPER, LOWER):
        add(rows_buf, col_of(0), col_of(0, 1), half, partner, 0, 1)
    for place in range(7):
        for step in (1, -1):
            dz, rows, _ = depth_queue(step)[place]
            add(
                rows_buf, col_of(dz - step), col_of(dz - step, 1), rows, partner,
                DEPTH_ARRIVAL[place], DEPTH_ARRIVAL[place] + 1,
            )

    def send(event):
        for leaves, _, out, _ in copies:
            if leaves == event:
                out.start()

    def receive(event):
        for _, arrives, _, into in copies:
            if arrives == event:
                into.wait_recv()

    def share(buf, sends, recvs, along_row):
        def out(i):
            if along_row:
                target, slot = (lax.rem(me_row + i, GROUP), me_col), me_row
            else:
                target, slot = (me_row, lax.rem(me_col + i, GROUP)), me_col
            return pltpu.make_async_remote_copy(
                src_ref=buf.at[slot], dst_ref=buf.at[slot], send_sem=sends.at[i], recv_sem=recvs.at[i],
                device_id=target, device_id_type=MESH,
            )

        def into(i):
            if along_row:
                target, slot = (lax.rem(me_row + i, GROUP), me_col), lax.rem(me_row + GROUP - i, GROUP)
            else:
                target, slot = (me_row, lax.rem(me_col + i, GROUP)), lax.rem(me_col + GROUP - i, GROUP)
            return pltpu.make_async_remote_copy(
                src_ref=buf.at[slot], dst_ref=buf.at[slot], send_sem=sends.at[i], recv_sem=recvs.at[i],
                device_id=target, device_id_type=MESH,
            )

        def start(i, carry):
            out(i).start()
            return carry

        def arrive(i, carry):
            into(i).wait_recv()
            return carry

        def finish(i, carry):
            out(i).wait_send()
            return carry

        return tuple(functools.partial(lax.fori_loop, 1, GROUP, f, 0) for f in (start, arrive, finish))

    part_start, part_arrive, part_finish = share(part_buf, part_send, part_recv, True)
    sum_start, sum_arrive, sum_finish = share(sum_buf, sum_send, sum_recv, False)
    tot_start, tot_arrive, tot_finish = share(tot_buf, tot_send, tot_recv, True)

    for load in loads:
        load.wait()
    for j in range(TILES):
        cols = slice(j * TB, (j + 1) * TB)
        part = jnp.zeros((1, TB), jnp.float32)
        for i in range(TILES):
            rows = slice(i * TB, (i + 1) * TB)
            tile = own[rows, cols].astype(jnp.float32) * tile_ref[i, j].astype(jnp.float32)
            part += jnp.sum(tile, axis=0, keepdims=True)
            rows_buf[me_col, rows, cols] = tile.astype(jnp.bfloat16)
            cols_buf[me_row, rows, cols] = tile.astype(jnp.bfloat16)
        part_buf[me_row, :, cols] = part
    acc[...] = jnp.zeros_like(acc)

    pl.semaphore_wait(barrier, 2 * (GROUP - 1))
    part_start()
    send(0)

    part_arrive()
    sums = part_buf[0]
    for i in range(1, GROUP):
        sums += part_buf[i]
    sum_buf[me_col] = sums
    part_finish()
    receive(1)
    sum_start()
    send(1)

    def multiply(stage):
        def one(k, carry):
            dx = wrap(lax.div(k, SIDE) - x, SIDE)
            dy = wrap(lax.rem(k, SIDE) - y, SIDE)
            dz = wrap(lax.div(k, 2) - z, DEPTH)

            def far(d):
                return lax.div(d * (SIDE - d), 4)

            def off(d):
                return lax.div(d + 3, 4)

            n = (far(dx) + far(dy)) * off(dx) * off(dy)
            by_plane = n + lax.div(n + 1, 2)
            reach = dz * (DEPTH - dz)
            by_depth = lax.div(reach, 15) + 2 * lax.div(reach, 16)

            @pl.when(jnp.maximum(by_plane, by_depth) == stage)
            def _():
                acc[...] += jnp.dot(rows_buf[k], cols_buf[k], preferred_element_type=jnp.float32)

            return carry

        lax.fori_loop(0, GROUP, one, 0)

    for event in range(2, EVENTS):
        receive(event)
        send(event)
        if event == 8:
            sum_arrive()

            def augment(k, carry):
                s = sum_buf[k]
                high = s.astype(jnp.bfloat16).astype(jnp.float32)
                rest = s - high
                mid = rest.astype(jnp.bfloat16).astype(jnp.float32)
                low = rest - mid
                index = lax.broadcasted_iota(jnp.int32, (AUG, BLOCK), 0)
                rows = jnp.where(index == 0, high, jnp.where(index == 1, mid, jnp.where(index == 2, low, 0.0)))
                rows_buf[k, BLOCK:, :] = rows.astype(jnp.bfloat16)
                return carry

            lax.fori_loop(0, GROUP, augment, 0)
        stage = {8: 0, 10: 1, 11: 2, 12: 3}.get(event)
        if stage is not None:
            multiply(stage)

    means = (acc[BLOCK : BLOCK + 1, :] + acc[BLOCK + 1 : BLOCK + 2, :] + acc[BLOCK + 2 : BLOCK + 3, :]) / ORDER
    cut = 0.125 * thr_ref[...].astype(jnp.float32) * means
    for j in range(TILES):
        cols = slice(j * TB, (j + 1) * TB)
        part = jnp.zeros((1, TB), jnp.float32)
        for i in range(TILES):
            rows = slice(i * TB, (i + 1) * TB)
            tile = jnp.maximum(acc[rows, cols] - cut[:, cols], 0.0) * keep_ref[i, j].astype(jnp.float32)
            pruned_ref[rows, cols] = tile
            part += jnp.sum(tile, axis=0, keepdims=True)
        tot_buf[me_row, :, cols] = part
    for _, _, out, _ in copies:
        out.wait_send()
    tot_start()
    sum_finish()
    tot_arrive()
    totals = tot_buf[0]
    for i in range(1, GROUP):
        totals += tot_buf[i]
    total_ref[...] = totals
    tot_finish()


def n_copies():
    return 40 + 14 + 16


def on_device(values, tile_mask, keep_mask, thr_index):
    vmem = pl.BlockSpec(memory_space=pltpu.VMEM)
    hbm = pl.BlockSpec(memory_space=pltpu.HBM)
    dma = pltpu.SemaphoreType.DMA
    pruned, totals = pl.pallas_call(
        kernel,
        out_shape=(
            jax.ShapeDtypeStruct((BLOCK, BLOCK), jnp.float32),
            jax.ShapeDtypeStruct((1, BLOCK), jnp.float32),
        ),
        in_specs=[hbm, hbm, hbm, hbm],
        out_specs=(vmem, vmem),
        scratch_shapes=[
            pltpu.SMEM((TILES, TILES), jnp.int32),
            pltpu.SMEM((TILES, TILES), jnp.int32),
            pltpu.VMEM((1, BLOCK), jnp.int32),
            pltpu.VMEM((GROUP, BLOCK + AUG, BLOCK), jnp.bfloat16),
            pltpu.VMEM((GROUP, BLOCK, BLOCK), jnp.bfloat16),
            pltpu.VMEM((BLOCK + AUG, BLOCK), jnp.float32),
            pltpu.VMEM((BLOCK, BLOCK), jnp.bfloat16),
            pltpu.VMEM((GROUP, 1, BLOCK), jnp.float32),
            pltpu.VMEM((GROUP, 1, BLOCK), jnp.float32),
            pltpu.VMEM((GROUP, 1, BLOCK), jnp.float32),
            dma((4,)), dma((n_copies(),)), dma((n_copies(),)),
            dma((GROUP,)), dma((GROUP,)), dma((GROUP,)), dma((GROUP,)), dma((GROUP,)), dma((GROUP,)),
        ],
        compiler_params=pltpu.CompilerParams(
            collective_id=0, has_side_effects=True, vmem_limit_bytes=40 * 1024 * 1024
        ),
        cost_estimate=pl.CostEstimate(
            flops=2 * BLOCK * BLOCK * ORDER, bytes_accessed=2 * 1024 * 1024, transcendentals=0
        ),
        name="expand",
    )(*(pltpu.with_memory_space_constraint(a, pltpu.HBM) for a in (values, tile_mask, keep_mask, thr_index.reshape(1, BLOCK))))
    return (pruned / jnp.maximum(totals / ORDER, 0.1)).astype(jnp.bfloat16)


def solution(mesh):
    return jax.shard_map(
        on_device,
        mesh=mesh,
        in_specs=(P("row", "col"), P("row", "col"), P("row", "col"), P("col")),
        out_specs=P("row", "col"),
        check_vma=False,
    )
```

```python
import functools

import jax
import jax.numpy as jnp
from jax import lax
from jax.experimental import pallas as pl
from jax.experimental.pallas import tpu as pltpu
from jax.sharding import PartitionSpec as P

TB = 128
BLOCK = 512
HALF = BLOCK // 2
QUART = BLOCK // 4
TILES = BLOCK // TB
GROUP = 16
SIDE = 4
DEPTH = 8
ORDER = BLOCK * GROUP
AUG = 16
ROUNDS = 4
MESH = pl.DeviceIdType.MESH

UPPER, LOWER = (0, HALF), (HALF, HALF)


def quarter(half, step):
    return (half[0] + (0 if step > 0 else QUART), QUART)


def plane_queue(axis, step):
    def at(along, across):
        return (along, across) if axis == 0 else (across, along)

    first, second = (UPPER, LOWER) if axis == 0 else (LOWER, UPPER)
    return [
        (at(0, 0), first, 0, 2),
        (at(0, 0), second, 0, 4),
        (at(-step, 0), quarter(first, step), 2, 5),
        (at(0, -1), second, 2, 7),
        (at(0, 1), second, 2, 9),
        (at(-step, 0), quarter(second, step), 4, 10),
        (at(0, 2), second, 5, 12),
        (at(-step, -1), quarter(second, step), 7, 13),
        (at(-step, 1), quarter(second, step), 9, 14),
        (at(-step, 2), quarter(second, step), 12, 15),
    ]


def depth_queue(step):
    first, second = (UPPER, LOWER) if step > 0 else (LOWER, UPPER)
    return [
        (0, first, 0, 2.1, 9.2),
        (0, second, 0, 4.1, 9.2),
        (-step, first, 2.1, 6.1, 9.2),
        (-step, second, 4.1, 8.1, 9.2),
        (-2 * step, first, 6.1, 10.1, 13.2),
        (-2 * step, second, 8.1, 12.1, 13.2),
        (-3 * step, quarter(first, 1), 10.1, 13.1, 15.2),
        (-3 * step, quarter(first, -1), 10.1, 14.1, 15.2),
    ]


STAGE_AFTER = {9.2: 0, 10.1: 1, 12.1: 2, 13.2: 3, 14.1: 4, 15: 5, 15.2: 6}


def wrap(value, size):
    return lax.rem(value + size, size)


def kernel(
    values_ref, tile_hbm, keep_hbm, thr_hbm, pruned_ref, total_ref, tile_ref, keep_ref, thr_ref,
    rows_buf, cols_buf, acc, own, part_buf, sum_buf, tot_buf,
    in_sem, send_sem, recv_sem, part_send, part_recv, sum_send, sum_recv, tot_send, tot_recv, ready_sem, round_sem,
):
    me_row, me_col = lax.axis_index("row"), lax.axis_index("col")
    x, y = lax.div(me_row, SIDE), lax.rem(me_row, SIDE)
    z, core = lax.div(me_col, 2), lax.rem(me_col, 2)

    def row_of(dx, dy):
        return wrap(x + dx, SIDE) * SIDE + wrap(y + dy, SIDE)

    def col_of(dz, other=0):
        return wrap(z + dz, DEPTH) * 2 + (1 - core if other else core)

    loads = [
        pltpu.make_async_copy(out, into, in_sem.at[i])
        for i, (out, into) in enumerate(
            ((values_ref, own), (tile_hbm, tile_ref), (keep_hbm, keep_ref), (thr_hbm, thr_ref))
        )
    ]
    for load in loads:
        load.start()

    links = []
    for axis in (0, 1):
        for step in (1, -1):
            dx, dy = (step, 0) if axis == 0 else (0, step)
            mine = x if axis == 0 else y
            links.append(((row_of(dx, dy), me_col), wrap(mine + step, SIDE), mine))
    for step in (1, -1):
        links.append(((me_row, col_of(step)), wrap(z + step, DEPTH), z))
    partner = (me_row, col_of(0, 1))

    barrier = pltpu.get_barrier_semaphore()
    pl.semaphore_signal(barrier, inc=1, device_id=partner, device_id_type=MESH)
    lower = 1
    for neighbour, theirs, mine in links:
        lower += (theirs < mine).astype(jnp.int32)

        @pl.when(theirs > mine)
        def _(neighbour=neighbour):
            pl.semaphore_signal(barrier, inc=1, device_id=neighbour, device_id_type=MESH)

    copies = []

    def copy_of(buf, slot, rows, number, target):
        part = buf.at[slot, pl.ds(*rows), :]
        return pltpu.make_async_remote_copy(
            src_ref=part, dst_ref=part, send_sem=send_sem.at[number], recv_sem=recv_sem.at[number],
            device_id=target, device_id_type=MESH,
        )

    def add(buf, sent_slot, got_slot, rows, target, leaves, arrives, link=None):
        number = len(copies)
        copies.append((
            leaves, arrives, link,
            copy_of(buf, sent_slot, rows, number, target),
            copy_of(buf, got_slot, rows, number, target),
        ))

    for place in range(10):
        for axis in (0, 1):
            for step in (1, -1):
                (dx, dy), rows, leaves, arrives = plane_queue(axis, step)[place]
                sx, sy = (step, 0) if axis == 0 else (0, step)
                add(
                    cols_buf, row_of(dx, dy), row_of(dx - sx, dy - sy), rows,
                    (row_of(sx, sy), me_col), leaves, arrives, 2 * axis + (step < 0),
                )
        if place < 8:
            for step in (1, -1):
                dz, rows, leaves, arrives, _ = depth_queue(step)[place]
                add(
                    rows_buf, col_of(dz), col_of(dz - step), rows,
                    (me_row, col_of(step)), leaves, arrives, 4 + (step < 0),
                )
    for half in (UPPER, LOWER):
        add(rows_buf, col_of(0), col_of(0, 1), half, partner, 0, 9.2)
    for place in range(8):
        for step in (1, -1):
            dz, rows, _, arrives, other = depth_queue(step)[place]
            add(rows_buf, col_of(dz - step), col_of(dz - step, 1), rows, partner, arrives, other)

    def send(event, link=None):
        for leaves, _, on, out, _ in copies:
            if leaves == event and (event > 0 or on == link):
                out.start()

    def receive(event):
        for _, arrives, _, _, into in copies:
            if arrives == event:
                into.wait_recv()

    def spread(number):
        for neighbour in [partner] + [link[0] for link in links]:
            pl.semaphore_signal(round_sem.at[number], inc=1, device_id=neighbour, device_id_type=MESH)
        pl.semaphore_wait(round_sem.at[number], len(links) + 1)

    def share(buf, sends, recvs, along_row):
        def out(i):
            if along_row:
                target, slot = (lax.rem(me_row + i, GROUP), me_col), me_row
            else:
                target, slot = (me_row, lax.rem(me_col + i, GROUP)), me_col
            return pltpu.make_async_remote_copy(
                src_ref=buf.at[slot], dst_ref=buf.at[slot], send_sem=sends.at[i], recv_sem=recvs.at[i],
                device_id=target, device_id_type=MESH,
            )

        def into(i):
            if along_row:
                target, slot = (lax.rem(me_row + i, GROUP), me_col), lax.rem(me_row + GROUP - i, GROUP)
            else:
                target, slot = (me_row, lax.rem(me_col + i, GROUP)), lax.rem(me_col + GROUP - i, GROUP)
            return pltpu.make_async_remote_copy(
                src_ref=buf.at[slot], dst_ref=buf.at[slot], send_sem=sends.at[i], recv_sem=recvs.at[i],
                device_id=target, device_id_type=MESH,
            )

        def start(i, carry):
            out(i).start()
            return carry

        def arrive(i, carry):
            into(i).wait_recv()
            return carry

        def finish(i, carry):
            out(i).wait_send()
            return carry

        return tuple(functools.partial(lax.fori_loop, 1, GROUP, f, 0) for f in (start, arrive, finish))

    part_start, part_arrive, part_finish = share(part_buf, part_send, part_recv, True)
    sum_start, sum_arrive, sum_finish = share(sum_buf, sum_send, sum_recv, False)
    tot_start, tot_arrive, tot_finish = share(tot_buf, tot_send, tot_recv, True)

    pl.semaphore_wait(barrier, lower)
    for number, (neighbour, theirs, mine) in enumerate(links):

        @pl.when(theirs < mine)
        def _(neighbour=neighbour, number=number):
            pl.semaphore_signal(ready_sem.at[number ^ 1], inc=1, device_id=neighbour, device_id_type=MESH)

    for load in loads:
        load.wait()
    for j in range(TILES):
        cols = slice(j * TB, (j + 1) * TB)
        part = jnp.zeros((1, TB), jnp.float32)
        for i in range(TILES):
            rows = slice(i * TB, (i + 1) * TB)
            tile = own[rows, cols].astype(jnp.float32) * tile_ref[i, j].astype(jnp.float32)
            part += jnp.sum(tile, axis=0, keepdims=True)
            rows_buf[me_col, rows, cols] = tile.astype(jnp.bfloat16)
            cols_buf[me_row, rows, cols] = tile.astype(jnp.bfloat16)
        part_buf[me_row, :, cols] = part
    acc[...] = jnp.zeros_like(acc)

    send(0)
    for number, (_, theirs, mine) in enumerate(links):

        @pl.when(theirs > mine)
        def _(number=number):
            pl.semaphore_wait(ready_sem.at[number], 1)

        send(0, number)

    for number in range(ROUNDS - 1):
        spread(number)
    part_start()

    def multiply(stage):
        def one(k, carry):
            dx = wrap(lax.div(k, SIDE) - x, SIDE)
            dy = wrap(lax.rem(k, SIDE) - y, SIDE)
            dz = wrap(lax.div(k, 2) - z, DEPTH)

            def far(d):
                return lax.div(d * (SIDE - d), 4)

            def off(d):
                return lax.div(d + 3, 4)

            n, both = far(dx) + far(dy), off(dx) * off(dy)
            slow = lax.rem(k + core, 2)
            by_plane = n * (2 - n) * (1 - both + both * lax.div(11 - dx - dy, 2)) + 5 * lax.div(n * (n - 1), 2)
            reach = dz * (DEPTH - dz)
            by_depth = lax.div(reach, 15) * (2 + slow) + lax.div(reach, 16) * (2 + slow)

            @pl.when(jnp.maximum(by_plane, by_depth) == stage)
            def _():
                acc[...] += jnp.dot(rows_buf[k], cols_buf[k], preferred_element_type=jnp.float32)

            return carry

        lax.fori_loop(0, GROUP, one, 0)

    for event in sorted({arrives for _, arrives, *_ in copies}):
        receive(event)
        send(event)
        if event == 2.1:
            spread(ROUNDS - 1)
        if event == 4.1:
            part_arrive()
            sums = part_buf[0]
            for i in range(1, GROUP):
                sums += part_buf[i]
            sum_buf[me_col] = sums
            part_finish()
            sum_start()
        if event == 9.2:
            sum_arrive()

            def augment(k, carry):
                s = sum_buf[k]
                high = s.astype(jnp.bfloat16).astype(jnp.float32)
                rest = s - high
                mid = rest.astype(jnp.bfloat16).astype(jnp.float32)
                low = rest - mid
                index = lax.broadcasted_iota(jnp.int32, (AUG, BLOCK), 0)
                rows = jnp.where(index == 0, high, jnp.where(index == 1, mid, jnp.where(index == 2, low, 0.0)))
                rows_buf[k, BLOCK:, :] = rows.astype(jnp.bfloat16)
                return carry

            lax.fori_loop(0, GROUP, augment, 0)
        if event in STAGE_AFTER:
            multiply(STAGE_AFTER[event])

    means = (acc[BLOCK : BLOCK + 1, :] + acc[BLOCK + 1 : BLOCK + 2, :] + acc[BLOCK + 2 : BLOCK + 3, :]) / ORDER
    cut = 0.125 * thr_ref[...].astype(jnp.float32) * means
    for j in range(TILES):
        cols = slice(j * TB, (j + 1) * TB)
        part = jnp.zeros((1, TB), jnp.float32)
        for i in range(TILES):
            rows = slice(i * TB, (i + 1) * TB)
            tile = jnp.maximum(acc[rows, cols] - cut[:, cols], 0.0) * keep_ref[i, j].astype(jnp.float32)
            pruned_ref[rows, cols] = tile
            part += jnp.sum(tile, axis=0, keepdims=True)
        tot_buf[me_row, :, cols] = part
    sum_finish()
    tot_start()
    for _, _, _, out, _ in copies:
        out.wait_send()
    tot_arrive()
    totals = tot_buf[0]
    for i in range(1, GROUP):
        totals += tot_buf[i]
    total_ref[...] = totals
    tot_finish()


def n_copies():
    return 40 + 16 + 2 + 16


def on_device(values, tile_mask, keep_mask, thr_index):
    vmem = pl.BlockSpec(memory_space=pltpu.VMEM)
    hbm = pl.BlockSpec(memory_space=pltpu.HBM)
    dma = pltpu.SemaphoreType.DMA
    pruned, totals = pl.pallas_call(
        kernel,
        out_shape=(
            jax.ShapeDtypeStruct((BLOCK, BLOCK), jnp.float32),
            jax.ShapeDtypeStruct((1, BLOCK), jnp.float32),
        ),
        in_specs=[hbm, hbm, hbm, hbm],
        out_specs=(vmem, vmem),
        scratch_shapes=[
            pltpu.SMEM((TILES, TILES), jnp.int32),
            pltpu.SMEM((TILES, TILES), jnp.int32),
            pltpu.VMEM((1, BLOCK), jnp.int32),
            pltpu.VMEM((GROUP, BLOCK + AUG, BLOCK), jnp.bfloat16),
            pltpu.VMEM((GROUP, BLOCK, BLOCK), jnp.bfloat16),
            pltpu.VMEM((BLOCK + AUG, BLOCK), jnp.float32),
            pltpu.VMEM((BLOCK, BLOCK), jnp.bfloat16),
            pltpu.VMEM((GROUP, 1, BLOCK), jnp.float32),
            pltpu.VMEM((GROUP, 1, BLOCK), jnp.float32),
            pltpu.VMEM((GROUP, 1, BLOCK), jnp.float32),
            dma((4,)), dma((n_copies(),)), dma((n_copies(),)),
            dma((GROUP,)), dma((GROUP,)), dma((GROUP,)), dma((GROUP,)), dma((GROUP,)), dma((GROUP,)),
            pltpu.SemaphoreType.REGULAR((6,)), pltpu.SemaphoreType.REGULAR((ROUNDS,)),
        ],
        compiler_params=pltpu.CompilerParams(
            collective_id=0, has_side_effects=True, vmem_limit_bytes=40 * 1024 * 1024
        ),
        cost_estimate=pl.CostEstimate(
            flops=2 * BLOCK * BLOCK * ORDER, bytes_accessed=2 * 1024 * 1024, transcendentals=0
        ),
        name="expand",
    )(*(pltpu.with_memory_space_constraint(a, pltpu.HBM) for a in (values, tile_mask, keep_mask, thr_index.reshape(1, BLOCK))))
    return (pruned / jnp.maximum(totals / ORDER, 0.1)).astype(jnp.bfloat16)


def solution(mesh):
    return jax.shard_map(
        on_device,
        mesh=mesh,
        in_specs=(P("row", "col"), P("row", "col"), P("row", "col"), P("col")),
        out_specs=P("row", "col"),
        check_vma=False,
    )
```

```python
import functools

import jax
import jax.numpy as jnp
from jax import lax
from jax.experimental import pallas as pl
from jax.experimental.pallas import tpu as pltpu
from jax.sharding import PartitionSpec as P

TB = 128
BLOCK = 512
HALF = BLOCK // 2
QUART = BLOCK // 4
TILES = BLOCK // TB
GROUP = 16
SIDE = 4
DEPTH = 8
ORDER = BLOCK * GROUP
AUG = 16
ROUNDS = 3
MESH = pl.DeviceIdType.MESH

UPPER, LOWER = (0, HALF), (HALF, HALF)


def quarter(half, step):
    return (half[0] + (0 if step > 0 else QUART), QUART)


def plane_queue(axis, step):
    def at(along, across):
        return (along, across) if axis == 0 else (across, along)

    first, second = (UPPER, LOWER) if axis == 0 else (LOWER, UPPER)
    return [
        (at(0, 0), first, 0, 2),
        (at(0, 0), second, 0, 4),
        (at(-step, 0), quarter(first, step), 2, 5),
        (at(0, -1), second, 2, 7),
        (at(0, 1), second, 2, 9),
        (at(-step, 0), quarter(second, step), 4, 10),
        (at(0, 2), second, 5, 12),
        (at(-step, -1), quarter(second, step), 7, 13),
        (at(-step, 1), quarter(second, step), 9, 14),
        (at(-step, 2), quarter(second, step), 12, 15),
    ]


SEAM = (192, 64)


def depth_queue(step):
    first, second = (UPPER, LOWER) if step > 0 else (LOWER, UPPER)
    last = ((0, 128), (128, 64)) if step > 0 else ((256, 128), (384, 128))
    return [
        (0, first, 0, 2.1),
        (0, second, 0, 4.1),
        (-step, first, 2.1, 6.1),
        (-step, second, 4.1, 8.1),
        (-2 * step, first, 6.1, 10.1),
        (-2 * step, second, 8.1, 12.1),
        (-3 * step, last[0], 10.1, 13.1),
        (-3 * step, last[1], 10.1, 14.1),
    ]


def chip_queue():
    moves = [(0, UPPER, 0, 9.2), (0, LOWER, 0, 9.2)]
    for step in (1, -1):
        first, second = (UPPER, LOWER) if step > 0 else (LOWER, UPPER)
        moves += [
            (-step, first, 2.1, 9.2),
            (-step, second, 4.1, 9.2),
            (-2 * step, first, 6.1, 9.2),
            (-2 * step, second, 8.1, 9.2),
            (-3 * step, first, 10.1, 14.2),
            (-3 * step, second, 12.1, 14.2),
            (-4 * step, quarter(first, 1), 13.1, 15.2),
            (-4 * step, quarter(first, -1), 14.1, 15.2),
        ]
    return sorted(moves, key=lambda move: move[2])


STAGE_AFTER = {10.1: (0, 1), 12.1: (2, 2), 13: (3, 3), 14.2: (4, 5)}


def wrap(value, size):
    return lax.rem(value + size, size)


def kernel(
    values_ref, tile_hbm, keep_hbm, thr_hbm, pruned_ref, total_ref, tile_ref, keep_ref, thr_ref,
    rows_buf, cols_buf, acc, own, part_buf, sum_buf, tot_buf,
    in_sem, send_sem, recv_sem, part_send, part_recv, sum_send, sum_recv, tot_send, tot_recv, over_send, over_recv,
    ready_sem, plane_sem, depth_sem,
):
    me_row, me_col = lax.axis_index("row"), lax.axis_index("col")
    x, y = lax.div(me_row, SIDE), lax.rem(me_row, SIDE)
    z, core = lax.div(me_col, 2), lax.rem(me_col, 2)

    def row_of(dx, dy):
        return wrap(x + dx, SIDE) * SIDE + wrap(y + dy, SIDE)

    def col_of(dz, other=0):
        return wrap(z + dz, DEPTH) * 2 + (1 - core if other else core)

    loads = [
        pltpu.make_async_copy(out, into, in_sem.at[i])
        for i, (out, into) in enumerate(
            ((values_ref, own), (tile_hbm, tile_ref), (keep_hbm, keep_ref), (thr_hbm, thr_ref))
        )
    ]
    for load in loads:
        load.start()

    links = []
    for axis in (0, 1):
        for step in (1, -1):
            dx, dy = (step, 0) if axis == 0 else (0, step)
            mine = x if axis == 0 else y
            links.append(((row_of(dx, dy), me_col), wrap(mine + step, SIDE), mine))
    for step in (1, -1):
        links.append(((me_row, col_of(step)), wrap(z + step, DEPTH), z))
    partner = (me_row, col_of(0, 1))

    barrier = pltpu.get_barrier_semaphore()
    pl.semaphore_signal(barrier, inc=1, device_id=partner, device_id_type=MESH)
    lower = 1
    for neighbour, theirs, mine in links:
        lower += (theirs < mine).astype(jnp.int32)

        @pl.when(theirs > mine)
        def _(neighbour=neighbour):
            pl.semaphore_signal(barrier, inc=1, device_id=neighbour, device_id_type=MESH)

    copies = []

    def copy_of(buf, slot, rows, number, target):
        above = AUG if buf is rows_buf else 0
        part = buf.at[slot, pl.ds(rows[0] + above, rows[1]), :]
        return pltpu.make_async_remote_copy(
            src_ref=part, dst_ref=part, send_sem=send_sem.at[number], recv_sem=recv_sem.at[number],
            device_id=target, device_id_type=MESH,
        )

    def add(buf, sent_slot, got_slot, rows, target, leaves, arrives, link=None):
        number = len(copies)
        copies.append((
            leaves, arrives, link,
            copy_of(buf, sent_slot, rows, number, target),
            copy_of(buf, got_slot, rows, number, target),
        ))

    for place in range(10):
        for axis in (0, 1):
            for step in (1, -1):
                (dx, dy), rows, leaves, arrives = plane_queue(axis, step)[place]
                sx, sy = (step, 0) if axis == 0 else (0, step)
                add(
                    cols_buf, row_of(dx, dy), row_of(dx - sx, dy - sy), rows,
                    (row_of(sx, sy), me_col), leaves, arrives, 2 * axis + (step < 0),
                )
        if place < 8:
            for step in (1, -1):
                dz, rows, leaves, arrives = depth_queue(step)[place]
                add(
                    rows_buf, col_of(dz), col_of(dz - step), rows,
                    (me_row, col_of(step)), leaves, arrives, 4 + (step < 0),
                )
    for dz, rows, leaves, arrives in chip_queue():
        add(rows_buf, col_of(dz), col_of(dz, 1), rows, partner, leaves, arrives)

    seam = len(copies)
    seam_up = copy_of(rows_buf, col_of(-3), SEAM, seam, (me_row, col_of(1)))
    seam_in = copy_of(rows_buf, col_of(4), SEAM, seam, (me_row, col_of(1)))
    part = rows_buf.at[col_of(3), pl.ds(SEAM[0] + AUG, SEAM[1]), :]
    seam_down = pltpu.make_async_remote_copy(
        src_ref=part, dst_ref=part, send_sem=send_sem.at[seam + 1], recv_sem=recv_sem.at[seam],
        device_id=(me_row, col_of(-1)), device_id_type=MESH,
    )

    def send(event, link=None, places=None):
        for leaves, arrives, on, out, _ in copies:
            if leaves == event and (event > 0 or on == link) and (places is None or arrives in places):
                out.start()
        if event == 10.1:

            @pl.when(z < DEPTH - 1)
            def _():
                seam_up.start()

        if event == 12.1:

            @pl.when(z == 1)
            def _():
                seam_down.start()

    def receive(event):
        for _, arrives, _, _, into in copies:
            if arrives == event:
                into.wait_recv()
        if event == 14.1:
            seam_in.wait_recv()

    def spread(sem, number, neighbours):
        for neighbour in neighbours:
            pl.semaphore_signal(sem.at[number], inc=1, device_id=neighbour, device_id_type=MESH)
        pl.semaphore_wait(sem.at[number], len(neighbours))

    def spread_depth(number):
        spread(depth_sem, number, [link[0] for link in links[4:]])

    def share(buf, sends, recvs, along_row):
        count = GROUP if along_row else DEPTH

        def slot_of(i):
            return lax.rem(me_row + i, GROUP) if along_row else wrap(z + i, DEPTH) * 2 + core

        def copy(i, slot):
            target = (slot_of(i), me_col) if along_row else (me_row, slot_of(i))
            return pltpu.make_async_remote_copy(
                src_ref=buf.at[slot], dst_ref=buf.at[slot], send_sem=sends.at[i], recv_sem=recvs.at[i],
                device_id=target, device_id_type=MESH,
            )

        def start(i, carry):
            copy(i, slot_of(0)).start()
            return carry

        def arrive(i, carry):
            copy(i, slot_of(count - i)).wait_recv()
            return carry

        def finish(i, carry):
            copy(i, slot_of(0)).wait_send()
            return carry

        return tuple(functools.partial(lax.fori_loop, 1, count, f, 0) for f in (start, arrive, finish))

    part_start, part_arrive, part_finish = share(part_buf, part_send, part_recv, True)
    sum_start, sum_arrive, sum_finish = share(sum_buf, sum_send, sum_recv, False)
    tot_start, tot_arrive, tot_finish = share(tot_buf, tot_send, tot_recv, True)

    def over(i, other):
        slot = wrap(z + i, DEPTH) * 2 + (1 - core if other else core)
        return pltpu.make_async_remote_copy(
            src_ref=sum_buf.at[slot], dst_ref=sum_buf.at[slot], send_sem=over_send.at[i], recv_sem=over_recv.at[i],
            device_id=partner, device_id_type=MESH,
        )

    def over_all(act):
        def one(i, carry):
            act(i)
            return carry

        lax.fori_loop(0, DEPTH, one, 0)

    pl.semaphore_wait(barrier, lower)
    for number, (neighbour, theirs, mine) in enumerate(links):

        @pl.when(theirs < mine)
        def _(neighbour=neighbour, number=number):
            pl.semaphore_signal(ready_sem.at[number ^ 1], inc=1, device_id=neighbour, device_id_type=MESH)

    for load in loads:
        load.wait()
    for j in range(TILES):
        cols = slice(j * TB, (j + 1) * TB)
        part = jnp.zeros((1, TB), jnp.float32)
        for i in range(TILES):
            rows = slice(i * TB, (i + 1) * TB)
            tile = own[rows, cols].astype(jnp.float32) * tile_ref[i, j].astype(jnp.float32)
            part += jnp.sum(tile, axis=0, keepdims=True)
            rows_buf[me_col, AUG + i * TB : AUG + (i + 1) * TB, cols] = tile.astype(jnp.bfloat16)
            cols_buf[me_row, rows, cols] = tile.astype(jnp.bfloat16)
        part_buf[me_row, :, cols] = part
    acc[...] = jnp.zeros_like(acc)

    def early(number):
        _, theirs, mine = links[number]

        @pl.when(theirs < mine)
        def _():
            send(0, number, (2,) if number < 4 else None)

    def late(number):
        _, theirs, mine = links[number]

        @pl.when(theirs > mine)
        def _():
            pl.semaphore_wait(ready_sem.at[number], 1)
            send(0, number, (2,) if number < 4 else None)

    for number in (4, 5, 0, 1, 2, 3):
        early(number)
    send(0)
    for number in range(5):
        late(number)
    for number in range(ROUNDS):
        spread(plane_sem, number, [link[0] for link in links[:4]])
    part_start()
    for number in range(4):
        send(0, number, (4,))
    late(5)
    spread_depth(0)

    def multiply(low, high):
        def one(k, carry):
            dx = wrap(lax.div(k, SIDE) - x, SIDE)
            dy = wrap(lax.rem(k, SIDE) - y, SIDE)
            dz = wrap(lax.div(k, 2) - z, DEPTH)

            def far(d):
                return lax.div(d * (SIDE - d), 4)

            def off(d):
                return lax.div(d + 3, 4)

            n, both = far(dx) + far(dy), off(dx) * off(dy)
            slow = lax.rem(k + core, 2)
            by_plane = n * (2 - n) * (1 - both + both * lax.div(11 - dx - dy, 2)) + 6 * lax.div(n * (n - 1), 2)
            reach = dz * (DEPTH - dz)
            by_depth = lax.div(reach, 15) * (2 + 2 * slow) + 3 * lax.div(reach, 16)

            ready = jnp.maximum(by_plane, by_depth)

            @pl.when((ready >= low) & (ready <= high))
            def _():
                acc[...] += jnp.dot(rows_buf[k], cols_buf[k], preferred_element_type=jnp.float32)

            return carry

        lax.fori_loop(0, GROUP, one, 0)

    for event in sorted({arrives for _, arrives, *_ in copies}):
        receive(event)
        send(event)
        if event == 2:
            spread_depth(1)
        if event == 2.1:
            spread_depth(2)
        if event == 4:
            part_arrive()
            sums = part_buf[0]
            for i in range(1, GROUP):
                sums += part_buf[i]
            sum_buf[me_col] = sums
            part_finish()
            sum_start()
        if event == 8.1:
            sum_arrive()
            over_all(lambda i: over(i, 0).start())
        if event == 9.2:
            over_all(lambda i: over(i, 1).wait_recv())

            def augment(k, carry):
                s = sum_buf[k]
                high = s.astype(jnp.bfloat16).astype(jnp.float32)
                rest = s - high
                mid = rest.astype(jnp.bfloat16).astype(jnp.float32)
                low = rest - mid
                index = lax.broadcasted_iota(jnp.int32, (AUG, BLOCK), 0)
                rows = jnp.where(index == 0, high, jnp.where(index == 1, mid, jnp.where(index == 2, low, 0.0)))
                rows_buf[k, :AUG, :] = rows.astype(jnp.bfloat16)
                return carry

            lax.fori_loop(0, GROUP, augment, 0)
        if event in STAGE_AFTER:
            multiply(*STAGE_AFTER[event])

    def product(k):
        return jnp.dot(rows_buf[k], cols_buf[k], preferred_element_type=jnp.float32)

    def finish(last):
        total = acc[...] + last
        means = (total[0:1] + total[1:2] + total[2:3]) / ORDER
        cut = 0.125 * thr_ref[...].astype(jnp.float32) * means
        for j in range(TILES):
            cols = slice(j * TB, (j + 1) * TB)
            part = jnp.zeros((1, TB), jnp.float32)
            for i in range(TILES):
                tile = total[AUG + i * TB : AUG + (i + 1) * TB, cols]
                tile = jnp.maximum(tile - cut[:, cols], 0.0) * keep_ref[i, j].astype(jnp.float32)
                pruned_ref[i * TB : (i + 1) * TB, cols] = tile
                part += jnp.sum(tile, axis=0, keepdims=True)
            tot_buf[me_row, :, cols] = part

    far_col, far_row = row_of(2, 2), col_of(4, 1)

    @pl.when(far_col != far_row)
    def _():
        acc[...] += product(far_col) + product(far_row)

    @pl.when(far_col == far_row)
    def _():
        acc[...] += product(far_col)

    finish(0.0)

    sum_finish()
    tot_start()
    for _, _, _, out, _ in copies:
        out.wait_send()
    over_all(lambda i: over(i, 0).wait_send())

    @pl.when(z < DEPTH - 1)
    def _():
        seam_up.wait_send()

    @pl.when(z == 1)
    def _():
        seam_down.wait_send()

    tot_arrive()
    totals = tot_buf[0]
    for i in range(1, GROUP):
        totals += tot_buf[i]
    total_ref[...] = totals
    tot_finish()


def n_copies():
    return 40 + 16 + 18 + 2


def on_device(values, tile_mask, keep_mask, thr_index):
    vmem = pl.BlockSpec(memory_space=pltpu.VMEM)
    hbm = pl.BlockSpec(memory_space=pltpu.HBM)
    dma = pltpu.SemaphoreType.DMA
    pruned, totals = pl.pallas_call(
        kernel,
        out_shape=(
            jax.ShapeDtypeStruct((BLOCK, BLOCK), jnp.float32),
            jax.ShapeDtypeStruct((1, BLOCK), jnp.float32),
        ),
        in_specs=[hbm, hbm, hbm, hbm],
        out_specs=(vmem, vmem),
        scratch_shapes=[
            pltpu.SMEM((TILES, TILES), jnp.int32),
            pltpu.SMEM((TILES, TILES), jnp.int32),
            pltpu.VMEM((1, BLOCK), jnp.int32),
            pltpu.VMEM((GROUP, BLOCK + AUG, BLOCK), jnp.bfloat16),
            pltpu.VMEM((GROUP, BLOCK, BLOCK), jnp.bfloat16),
            pltpu.VMEM((BLOCK + AUG, BLOCK), jnp.float32),
            pltpu.VMEM((BLOCK, BLOCK), jnp.bfloat16),
            pltpu.VMEM((GROUP, 1, BLOCK), jnp.float32),
            pltpu.VMEM((GROUP, 1, BLOCK), jnp.float32),
            pltpu.VMEM((GROUP, 1, BLOCK), jnp.float32),
            dma((4,)), dma((n_copies(),)), dma((n_copies(),)),
            dma((GROUP,)), dma((GROUP,)), dma((DEPTH,)), dma((DEPTH,)), dma((GROUP,)), dma((GROUP,)),
            dma((DEPTH,)), dma((DEPTH,)),
            pltpu.SemaphoreType.REGULAR((6,)), pltpu.SemaphoreType.REGULAR((ROUNDS,)), pltpu.SemaphoreType.REGULAR((ROUNDS,)),
        ],
        compiler_params=pltpu.CompilerParams(
            collective_id=0, has_side_effects=True, vmem_limit_bytes=40 * 1024 * 1024
        ),
        cost_estimate=pl.CostEstimate(
            flops=2 * BLOCK * BLOCK * ORDER, bytes_accessed=2 * 1024 * 1024, transcendentals=0
        ),
        name="expand",
    )(*(pltpu.with_memory_space_constraint(a, pltpu.HBM) for a in (values, tile_mask, keep_mask, thr_index.reshape(1, BLOCK))))
    return (pruned / jnp.maximum(totals / ORDER, 0.1)).astype(jnp.bfloat16)


def solution(mesh):
    return jax.shard_map(
        on_device,
        mesh=mesh,
        in_specs=(P("row", "col"), P("row", "col"), P("row", "col"), P("col")),
        out_specs=P("row", "col"),
        check_vma=False,
    )
```

```python
import functools

import jax
import jax.numpy as jnp
from jax import lax
from jax.experimental import pallas as pl
from jax.experimental.pallas import tpu as pltpu
from jax.sharding import PartitionSpec as P

TB = 128
BLOCK = 512
HALF = BLOCK // 2
QUART = BLOCK // 4
TILES = BLOCK // TB
GROUP = 16
SIDE = 4
DEPTH = 8
ORDER = BLOCK * GROUP
AUG = 16
ROUNDS = 3
MESH = pl.DeviceIdType.MESH

UPPER, LOWER = (0, HALF), (HALF, HALF)


def quarter(half, step):
    return (half[0] + (0 if step > 0 else QUART), QUART)


def plane_queue(axis, step):
    def at(along, across):
        return (along, across) if axis == 0 else (across, along)

    first, second = (UPPER, LOWER) if axis == 0 else (LOWER, UPPER)
    return [
        (at(0, 0), first, 0, 2),
        (at(0, 0), second, 0, 4),
        (at(-step, 0), quarter(first, step), 2, 5),
        (at(0, -1), second, 2, 7),
        (at(0, 1), second, 2, 9),
        (at(-step, 0), quarter(second, step), 4, 10),
        (at(0, 2), second, 5, 12),
        (at(-step, -1), quarter(second, step), 7, 13),
        (at(-step, 1), quarter(second, step), 9, 14),
        (at(-step, 2), quarter(second, step), 12, 15),
    ]


SEAM = (192, 64)


def depth_queue(step):
    first, second = (UPPER, LOWER) if step > 0 else (LOWER, UPPER)
    last = ((0, 128), (128, 64)) if step > 0 else ((256, 128), (384, 128))
    return [
        (0, first, 0, 2.1),
        (0, second, 0, 4.1),
        (-step, first, 2.1, 6.1),
        (-step, second, 4.1, 8.1),
        (-2 * step, first, 6.1, 10.1),
        (-2 * step, second, 8.1, 12.1),
        (-3 * step, last[0], 10.1, 13.1),
        (-3 * step, last[1], 10.1, 14.1),
    ]


def chip_queue():
    moves = [(0, UPPER, 0, 9.2), (0, LOWER, 0, 9.2)]
    for step in (1, -1):
        first, second = (UPPER, LOWER) if step > 0 else (LOWER, UPPER)
        moves += [
            (-step, first, 2.1, 9.2),
            (-step, second, 4.1, 9.2),
            (-2 * step, first, 6.1, 9.2),
            (-2 * step, second, 8.1, 9.2),
            (-3 * step, first, 10.1, 14.2),
            (-3 * step, second, 12.1, 14.2),
            (-4 * step, quarter(first, 1), 13.1, 15.2),
            (-4 * step, quarter(first, -1), 14.1, 15.2),
        ]
    return sorted(moves, key=lambda move: move[2])


STAGE_AFTER = {10.1: (0, 1), 12.1: (2, 2), 13: (3, 3), 14.2: (4, 5)}


def wrap(value, size):
    return lax.rem(value + size, size)


def kernel(
    values_ref, tile_hbm, keep_hbm, thr_hbm, pruned_ref, scale_ref, tile_ref, keep_ref, thr_ref,
    rows_buf, cols_buf, acc, own, part_buf, sum_buf, tot_buf,
    in_sem, send_sem, recv_sem, part_send, part_recv, sum_send, sum_recv, tot_send, tot_recv, over_send, over_recv,
    ready_sem, plane_sem, depth_sem,
):
    me_row, me_col = lax.axis_index("row"), lax.axis_index("col")
    x, y = lax.div(me_row, SIDE), lax.rem(me_row, SIDE)
    z, core = lax.div(me_col, 2), lax.rem(me_col, 2)

    def row_of(dx, dy):
        return wrap(x + dx, SIDE) * SIDE + wrap(y + dy, SIDE)

    def col_of(dz, other=0):
        return wrap(z + dz, DEPTH) * 2 + (1 - core if other else core)

    loads = [
        pltpu.make_async_copy(out, into, in_sem.at[i])
        for i, (out, into) in enumerate(
            ((values_ref, own), (tile_hbm, tile_ref), (keep_hbm, keep_ref), (thr_hbm, thr_ref))
        )
    ]
    for load in loads:
        load.start()

    links = []
    for axis in (0, 1):
        for step in (1, -1):
            dx, dy = (step, 0) if axis == 0 else (0, step)
            mine = x if axis == 0 else y
            links.append(((row_of(dx, dy), me_col), wrap(mine + step, SIDE), mine))
    for step in (1, -1):
        links.append(((me_row, col_of(step)), wrap(z + step, DEPTH), z))
    partner = (me_row, col_of(0, 1))

    barrier = pltpu.get_barrier_semaphore()
    pl.semaphore_signal(barrier, inc=1, device_id=partner, device_id_type=MESH)
    lower = 1
    for neighbour, theirs, mine in links:
        lower += (theirs < mine).astype(jnp.int32)

        @pl.when(theirs > mine)
        def _(neighbour=neighbour):
            pl.semaphore_signal(barrier, inc=1, device_id=neighbour, device_id_type=MESH)

    copies = []

    def copy_of(buf, slot, rows, number, target):
        above = AUG if buf is rows_buf else 0
        part = buf.at[slot, pl.ds(rows[0] + above, rows[1]), :]
        return pltpu.make_async_remote_copy(
            src_ref=part, dst_ref=part, send_sem=send_sem.at[number], recv_sem=recv_sem.at[number],
            device_id=target, device_id_type=MESH,
        )

    def add(buf, sent_slot, got_slot, rows, target, leaves, arrives, link=None):
        number = len(copies)
        copies.append((
            leaves, arrives, link,
            copy_of(buf, sent_slot, rows, number, target),
            copy_of(buf, got_slot, rows, number, target),
        ))

    for place in range(10):
        for axis in (0, 1):
            for step in (1, -1):
                (dx, dy), rows, leaves, arrives = plane_queue(axis, step)[place]
                sx, sy = (step, 0) if axis == 0 else (0, step)
                add(
                    cols_buf, row_of(dx, dy), row_of(dx - sx, dy - sy), rows,
                    (row_of(sx, sy), me_col), leaves, arrives, 2 * axis + (step < 0),
                )
        if place < 8:
            for step in (1, -1):
                dz, rows, leaves, arrives = depth_queue(step)[place]
                add(
                    rows_buf, col_of(dz), col_of(dz - step), rows,
                    (me_row, col_of(step)), leaves, arrives, 4 + (step < 0),
                )
    for dz, rows, leaves, arrives in chip_queue():
        add(rows_buf, col_of(dz), col_of(dz, 1), rows, partner, leaves, arrives)

    seam = len(copies)
    seam_up = copy_of(rows_buf, col_of(-3), SEAM, seam, (me_row, col_of(1)))
    seam_in = copy_of(rows_buf, col_of(4), SEAM, seam, (me_row, col_of(1)))
    part = rows_buf.at[col_of(3), pl.ds(SEAM[0] + AUG, SEAM[1]), :]
    seam_down = pltpu.make_async_remote_copy(
        src_ref=part, dst_ref=part, send_sem=send_sem.at[seam + 1], recv_sem=recv_sem.at[seam],
        device_id=(me_row, col_of(-1)), device_id_type=MESH,
    )

    def send(event, link=None, places=None):
        for leaves, arrives, on, out, _ in copies:
            if leaves == event and (event > 0 or on == link) and (places is None or arrives in places):
                out.start()
        if event == 10.1:

            @pl.when(z < DEPTH - 1)
            def _():
                seam_up.start()

        if event == 12.1:

            @pl.when(z == 1)
            def _():
                seam_down.start()

    def receive(event):
        for _, arrives, _, _, into in copies:
            if arrives == event:
                into.wait_recv()
        if event == 14.1:
            seam_in.wait_recv()

    def spread(sem, number, neighbours):
        for neighbour in neighbours:
            pl.semaphore_signal(sem.at[number], inc=1, device_id=neighbour, device_id_type=MESH)
        pl.semaphore_wait(sem.at[number], len(neighbours))

    def spread_plane(number):
        spread(plane_sem, number, [link[0] for link in links[:4]])

    def spread_depth(number):
        spread(depth_sem, number, [link[0] for link in links[4:]])

    def share(buf, sends, recvs, along_row):
        count = GROUP if along_row else DEPTH

        def slot_of(i):
            return lax.rem(me_row + i, GROUP) if along_row else wrap(z + i, DEPTH) * 2 + core

        def copy(i, slot):
            target = (slot_of(i), me_col) if along_row else (me_row, slot_of(i))
            return pltpu.make_async_remote_copy(
                src_ref=buf.at[slot], dst_ref=buf.at[slot], send_sem=sends.at[i], recv_sem=recvs.at[i],
                device_id=target, device_id_type=MESH,
            )

        def start(i, carry):
            copy(i, slot_of(0)).start()
            return carry

        def arrive(i, carry):
            copy(i, slot_of(count - i)).wait_recv()
            return carry

        def finish(i, carry):
            copy(i, slot_of(0)).wait_send()
            return carry

        return tuple(functools.partial(lax.fori_loop, 1, count, f, 0) for f in (start, arrive, finish))


    def part_copy(axis, d, slot):
        number = axis * SIDE + d
        return pltpu.make_async_remote_copy(
            src_ref=part_buf.at[axis * SIDE + slot], dst_ref=part_buf.at[axis * SIDE + slot],
            send_sem=part_send.at[number], recv_sem=part_recv.at[number],
            device_id=(row_of(0, d) if axis else row_of(d, 0), me_col), device_id_type=MESH,
        )

    def part_start(axis):
        for d in (2, 1, 3):
            part_copy(axis, d, y if axis else x).start()

    def part_finish(axis):
        for d in range(1, SIDE):
            part_copy(axis, d, y if axis else x).wait_send()

    def part_total(axis):
        for d in (1, 3, 2):
            part_copy(axis, d, wrap((y if axis else x) - d, SIDE)).wait_recv()
        slots = [part_buf[axis * SIDE + i] for i in range(SIDE)]
        return (slots[0] + slots[1]) + (slots[2] + slots[3])

    sum_start, sum_arrive, sum_finish = share(sum_buf, sum_send, sum_recv, False)
    tot_start, tot_arrive, tot_finish = share(tot_buf, tot_send, tot_recv, True)

    def over(i, other):
        slot = wrap(z + i, DEPTH) * 2 + (1 - core if other else core)
        return pltpu.make_async_remote_copy(
            src_ref=sum_buf.at[slot], dst_ref=sum_buf.at[slot], send_sem=over_send.at[i], recv_sem=over_recv.at[i],
            device_id=partner, device_id_type=MESH,
        )

    def over_all(act):
        def one(i, carry):
            act(i)
            return carry

        lax.fori_loop(0, DEPTH, one, 0)

    pl.semaphore_wait(barrier, lower)
    for number, (neighbour, theirs, mine) in enumerate(links):

        @pl.when(theirs < mine)
        def _(neighbour=neighbour, number=number):
            pl.semaphore_signal(ready_sem.at[number ^ 1], inc=1, device_id=neighbour, device_id_type=MESH)

    acc[...] = jnp.zeros_like(acc)
    for load in loads[:2]:
        load.wait()
    for j in range(TILES):
        cols = slice(j * TB, (j + 1) * TB)
        part = jnp.zeros((1, TB), jnp.float32)
        for i in range(TILES):
            rows = slice(i * TB, (i + 1) * TB)
            tile = own[rows, cols].astype(jnp.float32) * tile_ref[i, j].astype(jnp.float32)
            part += jnp.sum(tile, axis=0, keepdims=True)
            rows_buf[me_col, AUG + i * TB : AUG + (i + 1) * TB, cols] = tile.astype(jnp.bfloat16)
            cols_buf[me_row, rows, cols] = tile.astype(jnp.bfloat16)
        part_buf[x, :, cols] = part

    for load in loads[2:]:
        load.wait()

    def early(number):
        _, theirs, mine = links[number]

        @pl.when(theirs < mine)
        def _():
            send(0, number, (2,) if number < 4 else None)

    def late(number):
        _, theirs, mine = links[number]

        @pl.when(theirs > mine)
        def _():
            pl.semaphore_wait(ready_sem.at[number], 1)
            send(0, number, (2,) if number < 4 else None)

    for number in (4, 5, 0, 1, 2, 3):
        early(number)
    send(0)
    for number in range(5):
        late(number)
    spread_plane(0)
    part_start(0)
    for number in range(4):
        send(0, number, (4,))
    late(5)
    spread_depth(0)

    def multiply(low, high):
        def one(k, carry):
            dx = wrap(lax.div(k, SIDE) - x, SIDE)
            dy = wrap(lax.rem(k, SIDE) - y, SIDE)
            dz = wrap(lax.div(k, 2) - z, DEPTH)

            def far(d):
                return lax.div(d * (SIDE - d), 4)

            def off(d):
                return lax.div(d + 3, 4)

            n, both = far(dx) + far(dy), off(dx) * off(dy)
            slow = lax.rem(k + core, 2)
            by_plane = n * (2 - n) * (1 - both + both * lax.div(11 - dx - dy, 2)) + 6 * lax.div(n * (n - 1), 2)
            reach = dz * (DEPTH - dz)
            by_depth = lax.div(reach, 15) * (2 + 2 * slow) + 3 * lax.div(reach, 16)

            ready = jnp.maximum(by_plane, by_depth)

            @pl.when((ready >= low) & (ready <= high))
            def _():
                acc[...] += jnp.dot(rows_buf[k], cols_buf[k], preferred_element_type=jnp.float32)

            return carry

        lax.fori_loop(0, GROUP, one, 0)

    for event in sorted({arrives for _, arrives, *_ in copies}):
        receive(event)
        if event == 2:
            part_buf[SIDE + y] = part_total(0)
            part_finish(0)
            part_start(1)
        send(event)
        if event == 2:
            spread_depth(1)
        if event == 2.1:
            spread_depth(2)
        if event == 4:
            spread_plane(1)
        if event == 5:
            sum_buf[me_col] = part_total(1)
            part_finish(1)
            sum_start()
        if event == 7:
            spread_plane(2)
        if event == 9:
            sum_arrive()
            over_all(lambda i: over(i, 0).start())
        if event == 10.1:
            over_all(lambda i: over(i, 1).wait_recv())

            def augment(k, carry):
                s = sum_buf[k]
                high = s.astype(jnp.bfloat16).astype(jnp.float32)
                rest = s - high
                mid = rest.astype(jnp.bfloat16).astype(jnp.float32)
                low = rest - mid
                index = lax.broadcasted_iota(jnp.int32, (AUG, BLOCK), 0)
                rows = jnp.where(index == 0, high, jnp.where(index == 1, mid, jnp.where(index == 2, low, 0.0)))
                rows_buf[k, :AUG, :] = rows.astype(jnp.bfloat16)
                return carry

            lax.fori_loop(0, GROUP, augment, 0)
        if event in STAGE_AFTER:
            multiply(*STAGE_AFTER[event])

    def product(k):
        return jnp.dot(rows_buf[k], cols_buf[k], preferred_element_type=jnp.float32)

    def finish(last):
        total = acc[...] + last
        means = (total[0:1] + total[1:2] + total[2:3]) / ORDER
        cut = 0.125 * thr_ref[...].astype(jnp.float32) * means
        for j in range(TILES):
            cols = slice(j * TB, (j + 1) * TB)
            part = jnp.zeros((1, TB), jnp.float32)
            for i in range(TILES):
                tile = total[AUG + i * TB : AUG + (i + 1) * TB, cols]
                tile = jnp.maximum(tile - cut[:, cols], 0.0) * keep_ref[i, j].astype(jnp.float32)
                pruned_ref[i * TB : (i + 1) * TB, cols] = tile
                part += jnp.sum(tile, axis=0, keepdims=True)
            tot_buf[me_row, :, cols] = part

    far_col, far_row = row_of(2, 2), col_of(4, 1)

    @pl.when(far_col != far_row)
    def _():
        acc[...] += product(far_col) + product(far_row)

    @pl.when(far_col == far_row)
    def _():
        acc[...] += product(far_col)

    finish(0.0)

    sum_finish()
    tot_start()
    for _, _, _, out, _ in copies:
        out.wait_send()
    over_all(lambda i: over(i, 0).wait_send())

    @pl.when(z < DEPTH - 1)
    def _():
        seam_up.wait_send()

    @pl.when(z == 1)
    def _():
        seam_down.wait_send()

    tot_arrive()
    totals = tot_buf[0]
    for i in range(1, GROUP):
        totals += tot_buf[i]
    scale_ref[...] = jnp.maximum(totals / ORDER, 0.1)
    tot_finish()


def n_copies():
    return 40 + 16 + 18 + 2


def on_device(values, tile_mask, keep_mask, thr_index):
    vmem = pl.BlockSpec(memory_space=pltpu.VMEM)
    hbm = pl.BlockSpec(memory_space=pltpu.HBM)
    dma = pltpu.SemaphoreType.DMA
    pruned, scale = pl.pallas_call(
        kernel,
        out_shape=(
            jax.ShapeDtypeStruct((BLOCK, BLOCK), jnp.float32),
            jax.ShapeDtypeStruct((1, BLOCK), jnp.float32),
        ),
        in_specs=[hbm, hbm, hbm, hbm],
        out_specs=(vmem, vmem),
        scratch_shapes=[
            pltpu.SMEM((TILES, TILES), jnp.int32),
            pltpu.SMEM((TILES, TILES), jnp.int32),
            pltpu.VMEM((1, BLOCK), jnp.int32),
            pltpu.VMEM((GROUP, BLOCK + AUG, BLOCK), jnp.bfloat16),
            pltpu.VMEM((GROUP, BLOCK, BLOCK), jnp.bfloat16),
            pltpu.VMEM((BLOCK + AUG, BLOCK), jnp.float32),
            pltpu.VMEM((BLOCK, BLOCK), jnp.bfloat16),
            pltpu.VMEM((2 * SIDE, 1, BLOCK), jnp.float32),
            pltpu.VMEM((GROUP, 1, BLOCK), jnp.float32),
            pltpu.VMEM((GROUP, 1, BLOCK), jnp.float32),
            dma((4,)), dma((n_copies(),)), dma((n_copies(),)),
            dma((2 * SIDE,)), dma((2 * SIDE,)), dma((DEPTH,)), dma((DEPTH,)), dma((GROUP,)), dma((GROUP,)),
            dma((DEPTH,)), dma((DEPTH,)),
            pltpu.SemaphoreType.REGULAR((6,)), pltpu.SemaphoreType.REGULAR((ROUNDS,)), pltpu.SemaphoreType.REGULAR((ROUNDS,)),
        ],
        compiler_params=pltpu.CompilerParams(
            collective_id=0, has_side_effects=True, vmem_limit_bytes=40 * 1024 * 1024
        ),
        cost_estimate=pl.CostEstimate(
            flops=2 * BLOCK * BLOCK * ORDER, bytes_accessed=2 * 1024 * 1024, transcendentals=0
        ),
        name="expand",
    )(*(pltpu.with_memory_space_constraint(a, pltpu.HBM) for a in (values, tile_mask, keep_mask, thr_index.reshape(1, BLOCK))))
    return (pruned / scale).astype(jnp.bfloat16)


def solution(mesh):
    return jax.shard_map(
        on_device,
        mesh=mesh,
        in_specs=(P("row", "col"), P("row", "col"), P("row", "col"), P("col")),
        out_specs=P("row", "col"),
        check_vma=False,
    )
```

```python
import functools

import jax
import jax.numpy as jnp
from jax import lax
from jax.experimental import pallas as pl
from jax.experimental.pallas import tpu as pltpu
from jax.sharding import PartitionSpec as P

TB = 128
BLOCK = 512
HALF = BLOCK // 2
QUART = BLOCK // 4
TILES = BLOCK // TB
GROUP = 16
SIDE = 4
DEPTH = 8
ORDER = BLOCK * GROUP
AUG = 16
ROUNDS = 3
MESH = pl.DeviceIdType.MESH

UPPER, LOWER = (0, HALF), (HALF, HALF)


def quarter(half, step):
    return (half[0] + (0 if step > 0 else QUART), QUART)


def plane_queue(axis, step):
    def at(along, across):
        return (along, across) if axis == 0 else (across, along)

    first, second = (UPPER, LOWER) if axis == 0 else (LOWER, UPPER)
    return [
        (at(0, 0), first, 0, 2),
        (at(0, 0), second, 0, 4),
        (at(-step, 0), quarter(first, step), 2, 5),
        (at(0, -1), second, 2, 7),
        (at(0, 1), second, 2, 9),
        (at(-step, 0), quarter(second, step), 4, 10),
        (at(0, 2), second, 5, 12),
        (at(-step, -1), quarter(second, step), 7, 13),
        (at(-step, 1), quarter(second, step), 9, 14),
        (at(-step, 2), quarter(second, step), 12, 15),
    ]


SEAM = (192, 64)


def depth_queue(step):
    first, second = (UPPER, LOWER) if step > 0 else (LOWER, UPPER)
    last = ((0, 128), (128, 64)) if step > 0 else ((256, 128), (384, 128))
    return [
        (0, first, 0, 2.1),
        (0, second, 0, 4.1),
        (-step, first, 2.1, 6.1),
        (-step, second, 4.1, 8.1),
        (-2 * step, first, 6.1, 10.1),
        (-2 * step, second, 8.1, 12.1),
        (-3 * step, last[0], 10.1, 13.1 if step > 0 else 13.08),
        (-3 * step, last[1], 10.1, 14.1 if step > 0 else 14.08),
    ]


def chip_queue():
    moves = [(0, UPPER, 0, 9.2), (0, LOWER, 0, 9.2)]
    for step in (1, -1):
        first, second = (UPPER, LOWER) if step > 0 else (LOWER, UPPER)
        moves += [
            (-step, first, 2.1, 9.2),
            (-step, second, 4.1, 9.2),
            (-2 * step, first, 6.1, 9.2),
            (-2 * step, second, 8.1, 9.2),
            (-3 * step, first, 10.1, 14.2),
            (-3 * step, second, 12.1, 14.2),
            (-4 * step, quarter(first, 1), 13.1 if step > 0 else 13.08, 15.2),
            (-4 * step, quarter(first, -1), 14.1 if step > 0 else 14.08, 15.2),
        ]
    return sorted(moves, key=lambda move: move[2])


STAGE_AFTER = {12.1: (2, 2), 13: (3, 3), 14.2: (4, 5)}


def wrap(value, size):
    return lax.rem(value + size, size)


def kernel(
    values_ref, tile_hbm, keep_hbm, thr_hbm, pruned_ref, scale_ref, tile_ref, keep_ref, thr_ref,
    rows_buf, cols_buf, acc, own, part_buf, sum_buf, tot_buf,
    in_sem, send_sem, recv_sem, part_send, part_recv, sum_send, sum_recv, tot_send, tot_recv, over_send, over_recv,
    ready_sem, plane_sem, depth_sem,
):
    me_row, me_col = lax.axis_index("row"), lax.axis_index("col")
    x, y = lax.div(me_row, SIDE), lax.rem(me_row, SIDE)
    z, core = lax.div(me_col, 2), lax.rem(me_col, 2)

    def row_of(dx, dy):
        return wrap(x + dx, SIDE) * SIDE + wrap(y + dy, SIDE)

    def col_of(dz, other=0):
        return wrap(z + dz, DEPTH) * 2 + (1 - core if other else core)

    loads = [
        pltpu.make_async_copy(out, into, in_sem.at[i])
        for i, (out, into) in enumerate(
            ((values_ref, own), (tile_hbm, tile_ref), (keep_hbm, keep_ref), (thr_hbm, thr_ref))
        )
    ]
    for load in loads:
        load.start()

    links = []
    for axis in (0, 1):
        for step in (1, -1):
            dx, dy = (step, 0) if axis == 0 else (0, step)
            mine = x if axis == 0 else y
            links.append(((row_of(dx, dy), me_col), wrap(mine + step, SIDE), mine))
    for step in (1, -1):
        links.append(((me_row, col_of(step)), wrap(z + step, DEPTH), z))
    partner = (me_row, col_of(0, 1))

    barrier = pltpu.get_barrier_semaphore()
    pl.semaphore_signal(barrier, inc=1, device_id=partner, device_id_type=MESH)
    lower = 1
    for neighbour, theirs, mine in links:
        lower += (theirs < mine).astype(jnp.int32)

        @pl.when(theirs > mine)
        def _(neighbour=neighbour):
            pl.semaphore_signal(barrier, inc=1, device_id=neighbour, device_id_type=MESH)

    copies = []

    def copy_of(buf, slot, rows, number, target):
        above = AUG if buf is rows_buf else 0
        part = buf.at[slot, pl.ds(rows[0] + above, rows[1]), :]
        return pltpu.make_async_remote_copy(
            src_ref=part, dst_ref=part, send_sem=send_sem.at[number], recv_sem=recv_sem.at[number],
            device_id=target, device_id_type=MESH,
        )

    def add(buf, sent_slot, got_slot, rows, target, leaves, arrives, link=None):
        number = len(copies)
        copies.append((
            leaves, arrives, link,
            copy_of(buf, sent_slot, rows, number, target),
            copy_of(buf, got_slot, rows, number, target),
        ))

    for place in range(10):
        for axis in (0, 1):
            for step in (1, -1):
                (dx, dy), rows, leaves, arrives = plane_queue(axis, step)[place]
                sx, sy = (step, 0) if axis == 0 else (0, step)
                add(
                    cols_buf, row_of(dx, dy), row_of(dx - sx, dy - sy), rows,
                    (row_of(sx, sy), me_col), leaves, arrives, 2 * axis + (step < 0),
                )
        if place < 8:
            for step in (1, -1):
                dz, rows, leaves, arrives = depth_queue(step)[place]
                add(
                    rows_buf, col_of(dz), col_of(dz - step), rows,
                    (me_row, col_of(step)), leaves, arrives, 4 + (step < 0),
                )
    for dz, rows, leaves, arrives in chip_queue():
        add(rows_buf, col_of(dz), col_of(dz, 1), rows, partner, leaves, arrives)

    seam = len(copies)
    seam_up = copy_of(rows_buf, col_of(-3), SEAM, seam, (me_row, col_of(1)))
    seam_in = copy_of(rows_buf, col_of(4), SEAM, seam, (me_row, col_of(1)))
    part = rows_buf.at[col_of(3), pl.ds(SEAM[0] + AUG, SEAM[1]), :]
    seam_down = pltpu.make_async_remote_copy(
        src_ref=part, dst_ref=part, send_sem=send_sem.at[seam + 1], recv_sem=recv_sem.at[seam],
        device_id=(me_row, col_of(-1)), device_id_type=MESH,
    )

    def send(event, link=None, places=None):
        for leaves, arrives, on, out, _ in copies:
            if leaves == event and (event > 0 or on == link) and (places is None or arrives in places):
                out.start()
        if event == 10.1:

            @pl.when(z < DEPTH - 1)
            def _():
                seam_up.start()

        if event == 12.1:

            @pl.when(z == 1)
            def _():
                seam_down.start()

    def receive(event):
        for _, arrives, _, _, into in copies:
            if arrives == event:
                into.wait_recv()
        if event == 14.1:
            seam_in.wait_recv()

    def spread(sem, number, neighbours):
        for neighbour in neighbours:
            pl.semaphore_signal(sem.at[number], inc=1, device_id=neighbour, device_id_type=MESH)
        pl.semaphore_wait(sem.at[number], len(neighbours))

    def spread_plane(number):
        spread(plane_sem, number, [link[0] for link in links[:4]])

    def spread_depth(number):
        spread(depth_sem, number, [link[0] for link in links[4:]])

    def share(buf, sends, recvs, along_row):
        count = GROUP if along_row else DEPTH

        def slot_of(i):
            return lax.rem(me_row + i, GROUP) if along_row else wrap(z + i, DEPTH) * 2 + core

        def copy(i, slot):
            target = (slot_of(i), me_col) if along_row else (me_row, slot_of(i))
            return pltpu.make_async_remote_copy(
                src_ref=buf.at[slot], dst_ref=buf.at[slot], send_sem=sends.at[i], recv_sem=recvs.at[i],
                device_id=target, device_id_type=MESH,
            )

        def start(i, carry):
            copy(i, slot_of(0)).start()
            return carry

        def arrive(i, carry):
            copy(i, slot_of(count - i)).wait_recv()
            return carry

        def finish(i, carry):
            copy(i, slot_of(0)).wait_send()
            return carry

        return tuple(functools.partial(lax.fori_loop, 1, count, f, 0) for f in (start, arrive, finish))


    def part_copy(axis, d, slot):
        number = axis * SIDE + d
        return pltpu.make_async_remote_copy(
            src_ref=part_buf.at[axis * SIDE + slot], dst_ref=part_buf.at[axis * SIDE + slot],
            send_sem=part_send.at[number], recv_sem=part_recv.at[number],
            device_id=(row_of(0, d) if axis else row_of(d, 0), me_col), device_id_type=MESH,
        )

    def part_start(axis):
        for d in (2, 1, 3):
            part_copy(axis, d, y if axis else x).start()

    def part_finish(axis):
        for d in range(1, SIDE):
            part_copy(axis, d, y if axis else x).wait_send()

    def part_total(axis):
        for d in (1, 3, 2):
            part_copy(axis, d, wrap((y if axis else x) - d, SIDE)).wait_recv()
        slots = [part_buf[axis * SIDE + i] for i in range(SIDE)]
        return (slots[0] + slots[1]) + (slots[2] + slots[3])

    sum_start, sum_arrive, sum_finish = share(sum_buf, sum_send, sum_recv, False)
    tot_start, tot_arrive, tot_finish = share(tot_buf, tot_send, tot_recv, True)

    def over(i, other):
        slot = wrap(z + i, DEPTH) * 2 + (1 - core if other else core)
        return pltpu.make_async_remote_copy(
            src_ref=sum_buf.at[slot], dst_ref=sum_buf.at[slot], send_sem=over_send.at[i], recv_sem=over_recv.at[i],
            device_id=partner, device_id_type=MESH,
        )

    def over_all(act):
        def one(i, carry):
            act(i)
            return carry

        lax.fori_loop(0, DEPTH, one, 0)

    pl.semaphore_wait(barrier, lower)
    for number, (neighbour, theirs, mine) in enumerate(links):

        @pl.when(theirs < mine)
        def _(neighbour=neighbour, number=number):
            pl.semaphore_signal(ready_sem.at[number ^ 1], inc=1, device_id=neighbour, device_id_type=MESH)

    acc[...] = jnp.zeros_like(acc)
    for load in loads[:2]:
        load.wait()
    for j in range(TILES):
        cols = slice(j * TB, (j + 1) * TB)
        part = jnp.zeros((1, TB), jnp.float32)
        for i in range(TILES):
            rows = slice(i * TB, (i + 1) * TB)
            tile = own[rows, cols].astype(jnp.float32) * tile_ref[i, j].astype(jnp.float32)
            part += jnp.sum(tile, axis=0, keepdims=True)
            rows_buf[me_col, AUG + i * TB : AUG + (i + 1) * TB, cols] = tile.astype(jnp.bfloat16)
            cols_buf[me_row, rows, cols] = tile.astype(jnp.bfloat16)
        part_buf[x, :, cols] = part

    for load in loads[2:]:
        load.wait()

    def early(number):
        _, theirs, mine = links[number]

        @pl.when(theirs < mine)
        def _():
            send(0, number, (2,) if number < 4 else None)

    def late(number):
        _, theirs, mine = links[number]

        @pl.when(theirs > mine)
        def _():
            pl.semaphore_wait(ready_sem.at[number], 1)
            send(0, number, (2,) if number < 4 else None)

    for number in (4, 5, 0, 1, 2, 3):
        early(number)
    send(0)
    for number in range(5):
        late(number)
    spread_plane(0)
    part_start(0)
    for number in range(4):
        send(0, number, (4,))
    late(5)
    spread_depth(0)

    def multiply(low, high):
        def one(k, carry):
            dx = wrap(lax.div(k, SIDE) - x, SIDE)
            dy = wrap(lax.rem(k, SIDE) - y, SIDE)
            dz = wrap(lax.div(k, 2) - z, DEPTH)

            def far(d):
                return lax.div(d * (SIDE - d), 4)

            def off(d):
                return lax.div(d + 3, 4)

            n, both = far(dx) + far(dy), off(dx) * off(dy)
            slow = lax.rem(k + core, 2)
            by_plane = n * (2 - n) * (1 - both + both * lax.div(11 - dx - dy, 2)) + 6 * lax.div(n * (n - 1), 2)
            reach = dz * (DEPTH - dz)
            by_depth = lax.div(reach, 15) * (2 + 2 * slow) + 3 * lax.div(reach, 16)

            ready = jnp.maximum(by_plane, by_depth)

            @pl.when((ready >= low) & (ready <= high))
            def _():
                acc[...] += jnp.dot(rows_buf[k], cols_buf[k], preferred_element_type=jnp.float32)

            return carry

        lax.fori_loop(0, GROUP, one, 0)

    for event in sorted({arrives for _, arrives, *_ in copies}):
        receive(event)
        if event == 2:
            part_buf[SIDE + y] = part_total(0)
            part_finish(0)
            part_start(1)
        send(event)
        if event == 2:
            spread_depth(1)
        if event == 2.1:
            spread_depth(2)
        if event == 4:
            spread_plane(1)
        if event == 5:
            sum_buf[me_col] = part_total(1)
            part_finish(1)
            sum_start()
        if event == 7:
            spread_plane(2)
        if event == 9:
            sum_arrive()
            over_all(lambda i: over(i, 0).start())
        if event == 10.1:
            over_all(lambda i: over(i, 1).wait_recv())

            def augment(k, carry):
                s = sum_buf[k]
                high = s.astype(jnp.bfloat16).astype(jnp.float32)
                rest = s - high
                mid = rest.astype(jnp.bfloat16).astype(jnp.float32)
                low = rest - mid
                index = lax.broadcasted_iota(jnp.int32, (AUG, BLOCK), 0)
                rows = jnp.where(index == 0, high, jnp.where(index == 1, mid, jnp.where(index == 2, low, 0.0)))
                rows_buf[k, :AUG, :] = rows.astype(jnp.bfloat16)
                return carry

            lax.fori_loop(0, GROUP, augment, 0)
        if event in (10.1, 12):
            pl.when(z > 0 if event == 10.1 else z == 0)(functools.partial(multiply, 0, 1))
        if event in STAGE_AFTER:
            multiply(*STAGE_AFTER[event])

    def product(k):
        return jnp.dot(rows_buf[k], cols_buf[k], preferred_element_type=jnp.float32)

    def finish(last):
        total = acc[...] + last
        means = (total[0:1] + total[1:2] + total[2:3]) / ORDER
        cut = 0.125 * thr_ref[...].astype(jnp.float32) * means
        for j in range(TILES):
            cols = slice(j * TB, (j + 1) * TB)
            part = jnp.zeros((1, TB), jnp.float32)
            for i in range(TILES):
                tile = total[AUG + i * TB : AUG + (i + 1) * TB, cols]
                tile = jnp.maximum(tile - cut[:, cols], 0.0) * keep_ref[i, j].astype(jnp.float32)
                pruned_ref[i * TB : (i + 1) * TB, cols] = tile
                part += jnp.sum(tile, axis=0, keepdims=True)
            tot_buf[me_row, :, cols] = part

    far_col, far_row = row_of(2, 2), col_of(4, 1)

    @pl.when(far_col != far_row)
    def _():
        acc[...] += product(far_col) + product(far_row)

    @pl.when(far_col == far_row)
    def _():
        acc[...] += product(far_col)

    finish(0.0)

    sum_finish()
    tot_start()
    for _, _, _, out, _ in copies:
        out.wait_send()
    over_all(lambda i: over(i, 0).wait_send())

    @pl.when(z < DEPTH - 1)
    def _():
        seam_up.wait_send()

    @pl.when(z == 1)
    def _():
        seam_down.wait_send()

    tot_arrive()
    totals = tot_buf[0]
    for i in range(1, GROUP):
        totals += tot_buf[i]
    scale_ref[...] = jnp.maximum(totals / ORDER, 0.1)
    tot_finish()


def n_copies():
    return 40 + 16 + 18 + 2


def on_device(values, tile_mask, keep_mask, thr_index):
    vmem = pl.BlockSpec(memory_space=pltpu.VMEM)
    hbm = pl.BlockSpec(memory_space=pltpu.HBM)
    dma = pltpu.SemaphoreType.DMA
    pruned, scale = pl.pallas_call(
        kernel,
        out_shape=(
            jax.ShapeDtypeStruct((BLOCK, BLOCK), jnp.float32),
            jax.ShapeDtypeStruct((1, BLOCK), jnp.float32),
        ),
        in_specs=[hbm, hbm, hbm, hbm],
        out_specs=(vmem, vmem),
        scratch_shapes=[
            pltpu.SMEM((TILES, TILES), jnp.int32),
            pltpu.SMEM((TILES, TILES), jnp.int32),
            pltpu.VMEM((1, BLOCK), jnp.int32),
            pltpu.VMEM((GROUP, BLOCK + AUG, BLOCK), jnp.bfloat16),
            pltpu.VMEM((GROUP, BLOCK, BLOCK), jnp.bfloat16),
            pltpu.VMEM((BLOCK + AUG, BLOCK), jnp.float32),
            pltpu.VMEM((BLOCK, BLOCK), jnp.bfloat16),
            pltpu.VMEM((2 * SIDE, 1, BLOCK), jnp.float32),
            pltpu.VMEM((GROUP, 1, BLOCK), jnp.float32),
            pltpu.VMEM((GROUP, 1, BLOCK), jnp.float32),
            dma((4,)), dma((n_copies(),)), dma((n_copies(),)),
            dma((2 * SIDE,)), dma((2 * SIDE,)), dma((DEPTH,)), dma((DEPTH,)), dma((GROUP,)), dma((GROUP,)),
            dma((DEPTH,)), dma((DEPTH,)),
            pltpu.SemaphoreType.REGULAR((6,)), pltpu.SemaphoreType.REGULAR((ROUNDS,)), pltpu.SemaphoreType.REGULAR((ROUNDS,)),
        ],
        compiler_params=pltpu.CompilerParams(
            collective_id=0, has_side_effects=True, vmem_limit_bytes=40 * 1024 * 1024
        ),
        cost_estimate=pl.CostEstimate(
            flops=2 * BLOCK * BLOCK * ORDER, bytes_accessed=2 * 1024 * 1024, transcendentals=0
        ),
        name="expand",
    )(*(pltpu.with_memory_space_constraint(a, pltpu.HBM) for a in (values, tile_mask, keep_mask, thr_index.reshape(1, BLOCK))))
    return (pruned / scale).astype(jnp.bfloat16)


def solution(mesh):
    return jax.shard_map(
        on_device,
        mesh=mesh,
        in_specs=(P("row", "col"), P("row", "col"), P("row", "col"), P("col")),
        out_specs=P("row", "col"),
        check_vma=False,
    )
```

```python
import functools

import jax
import jax.numpy as jnp
from jax import lax
from jax.experimental import pallas as pl
from jax.experimental.pallas import tpu as pltpu
from jax.sharding import PartitionSpec as P

TB = 128
BLOCK = 512
HALF = BLOCK // 2
QUART = BLOCK // 4
TILES = BLOCK // TB
GROUP = 16
SIDE = 4
DEPTH = 8
ORDER = BLOCK * GROUP
AUG = 16
ROUNDS = 3
MESH = pl.DeviceIdType.MESH

UPPER, LOWER = (0, HALF), (HALF, HALF)


def quarter(half, step):
    return (half[0] + (0 if step > 0 else QUART), QUART)


def plane_queue(axis, step):
    def at(along, across):
        return (along, across) if axis == 0 else (across, along)

    first, second = (UPPER, LOWER) if axis == 0 else (LOWER, UPPER)
    return [
        (at(0, 0), first, 0, 2),
        (at(0, 0), second, 0, 4),
        (at(-step, 0), quarter(first, step), 2, 5),
        (at(0, -1), second, 2, 7),
        (at(0, 1), second, 2, 9),
        (at(-step, 0), quarter(second, step), 4, 10),
        (at(0, 2), second, 5, 12),
        (at(-step, -1), quarter(second, step), 7, 13),
        (at(-step, 1), quarter(second, step), 9, 14),
        (at(-step, 2), quarter(second, step), 12, 15),
    ]


SEAM = (192, 64)


def depth_queue(step):
    first, second = (UPPER, LOWER) if step > 0 else (LOWER, UPPER)
    last = ((0, 128), (128, 64)) if step > 0 else ((256, 128), (384, 128))
    return [
        (0, first, 0, 2.1),
        (0, second, 0, 4.1),
        (-step, first, 2.1, 6.1),
        (-step, second, 4.1, 8.1),
        (-2 * step, first, 6.1, 10.1),
        (-2 * step, second, 8.1, 12.1),
        (-3 * step, last[0], 10.1, 13.1 if step > 0 else 13.08),
        (-3 * step, last[1], 10.1, 14.1 if step > 0 else 14.08),
    ]


def chip_queue():
    moves = [(0, UPPER, 0, 9.2), (0, LOWER, 0, 9.2)]
    for step in (1, -1):
        first, second = (UPPER, LOWER) if step > 0 else (LOWER, UPPER)
        moves += [
            (-step, first, 2.1, 9.2),
            (-step, second, 4.1, 9.2),
            (-2 * step, first, 6.1, 9.2),
            (-2 * step, second, 8.1, 9.2),
            (-3 * step, first, 10.1, 14.2),
            (-3 * step, second, 12.1, 14.2),
            (-4 * step, quarter(first, 1), 13.1 if step > 0 else 13.08, 15.2),
            (-4 * step, quarter(first, -1), 14.1 if step > 0 else 14.08, 15.2),
        ]
    return sorted(moves, key=lambda move: move[2])


STAGE_AFTER = {12.1: (2, 2), 13: (3, 3), 14.2: (4, 5)}


def wrap(value, size):
    return lax.rem(value + size, size)


def kernel(
    values_ref, tile_hbm, keep_hbm, thr_hbm, pruned_ref, scale_ref, tile_ref, keep_ref, thr_ref,
    rows_buf, cols_buf, acc, own, part_buf, sum_buf, tot_buf,
    in_sem, send_sem, recv_sem, part_send, part_recv, sum_send, sum_recv, tot_send, tot_recv, over_send, over_recv,
    ready_sem, plane_sem, depth_sem,
):
    me_row, me_col = lax.axis_index("row"), lax.axis_index("col")
    x, y = lax.div(me_row, SIDE), lax.rem(me_row, SIDE)
    z, core = lax.div(me_col, 2), lax.rem(me_col, 2)

    def row_of(dx, dy):
        return wrap(x + dx, SIDE) * SIDE + wrap(y + dy, SIDE)

    def col_of(dz, other=0):
        return wrap(z + dz, DEPTH) * 2 + (1 - core if other else core)

    loads = [
        pltpu.make_async_copy(out, into, in_sem.at[i])
        for i, (out, into) in enumerate(
            ((values_ref, own), (tile_hbm, tile_ref), (keep_hbm, keep_ref), (thr_hbm, thr_ref))
        )
    ]
    for load in loads:
        load.start()

    links = []
    for axis in (0, 1):
        for step in (1, -1):
            dx, dy = (step, 0) if axis == 0 else (0, step)
            mine = x if axis == 0 else y
            links.append(((row_of(dx, dy), me_col), wrap(mine + step, SIDE), mine))
    for step in (1, -1):
        links.append(((me_row, col_of(step)), wrap(z + step, DEPTH), z))
    partner = (me_row, col_of(0, 1))

    barrier = pltpu.get_barrier_semaphore()
    pl.semaphore_signal(barrier, inc=1, device_id=partner, device_id_type=MESH)
    lower = 1
    for neighbour, theirs, mine in links:
        lower += (theirs < mine).astype(jnp.int32)

        @pl.when(theirs > mine)
        def _(neighbour=neighbour):
            pl.semaphore_signal(barrier, inc=1, device_id=neighbour, device_id_type=MESH)

    copies = []

    def copy_of(buf, slot, rows, number, target):
        above = AUG if buf is rows_buf else 0
        part = buf.at[slot, pl.ds(rows[0] + above, rows[1]), :]
        return pltpu.make_async_remote_copy(
            src_ref=part, dst_ref=part, send_sem=send_sem.at[number], recv_sem=recv_sem.at[number],
            device_id=target, device_id_type=MESH,
        )

    def add(buf, sent_slot, got_slot, rows, target, leaves, arrives, link=None):
        number = len(copies)
        copies.append((
            leaves, arrives, link,
            copy_of(buf, sent_slot, rows, number, target),
            copy_of(buf, got_slot, rows, number, target),
        ))

    for place in range(10):
        for axis in (0, 1):
            for step in (1, -1):
                (dx, dy), rows, leaves, arrives = plane_queue(axis, step)[place]
                sx, sy = (step, 0) if axis == 0 else (0, step)
                add(
                    cols_buf, row_of(dx, dy), row_of(dx - sx, dy - sy), rows,
                    (row_of(sx, sy), me_col), leaves, arrives, 2 * axis + (step < 0),
                )
        if place < 8:
            for step in (1, -1):
                dz, rows, leaves, arrives = depth_queue(step)[place]
                add(
                    rows_buf, col_of(dz), col_of(dz - step), rows,
                    (me_row, col_of(step)), leaves, arrives, 4 + (step < 0),
                )
    for dz, rows, leaves, arrives in chip_queue():
        add(rows_buf, col_of(dz), col_of(dz, 1), rows, partner, leaves, arrives)

    seam = len(copies)
    seam_up = copy_of(rows_buf, col_of(-3), SEAM, seam, (me_row, col_of(1)))
    seam_in = copy_of(rows_buf, col_of(4), SEAM, seam, (me_row, col_of(1)))
    part = rows_buf.at[col_of(3), pl.ds(SEAM[0] + AUG, SEAM[1]), :]
    seam_down = pltpu.make_async_remote_copy(
        src_ref=part, dst_ref=part, send_sem=send_sem.at[seam + 1], recv_sem=recv_sem.at[seam],
        device_id=(me_row, col_of(-1)), device_id_type=MESH,
    )

    def send(event, link=None, places=None):
        for leaves, arrives, on, out, _ in copies:
            if leaves == event and (event > 0 or on == link) and (places is None or arrives in places):
                out.start()
        if event == 10.1:

            @pl.when(z < DEPTH - 1)
            def _():
                seam_up.start()

        if event == 12.1:

            @pl.when(z == 1)
            def _():
                seam_down.start()

    def receive(event):
        for _, arrives, _, _, into in copies:
            if arrives == event:
                into.wait_recv()
        if event == 14.1:
            seam_in.wait_recv()

    def spread(sem, number, neighbours):
        for neighbour in neighbours:
            pl.semaphore_signal(sem.at[number], inc=1, device_id=neighbour, device_id_type=MESH)
        pl.semaphore_wait(sem.at[number], len(neighbours))

    def spread_plane(number):
        spread(plane_sem, number, [link[0] for link in links[:4]])

    def spread_depth(number):
        spread(depth_sem, number, [link[0] for link in links[4:]])

    def share(buf, sends, recvs, along_row):
        count = GROUP if along_row else DEPTH

        def slot_of(i):
            return lax.rem(me_row + i, GROUP) if along_row else wrap(z + i, DEPTH) * 2 + core

        def copy(i, slot):
            target = (slot_of(i), me_col) if along_row else (me_row, slot_of(i))
            return pltpu.make_async_remote_copy(
                src_ref=buf.at[slot], dst_ref=buf.at[slot], send_sem=sends.at[i], recv_sem=recvs.at[i],
                device_id=target, device_id_type=MESH,
            )

        def start(i, carry):
            copy(i, slot_of(0)).start()
            return carry

        def arrive(i, carry):
            copy(i, slot_of(count - i)).wait_recv()
            return carry

        def finish(i, carry):
            copy(i, slot_of(0)).wait_send()
            return carry

        return tuple(functools.partial(lax.fori_loop, 1, count, f, 0) for f in (start, arrive, finish))


    def part_copy(axis, d, slot):
        number = axis * SIDE + d
        return pltpu.make_async_remote_copy(
            src_ref=part_buf.at[axis * SIDE + slot], dst_ref=part_buf.at[axis * SIDE + slot],
            send_sem=part_send.at[number], recv_sem=part_recv.at[number],
            device_id=(row_of(0, d) if axis else row_of(d, 0), me_col), device_id_type=MESH,
        )

    def part_start(axis):
        for d in (2, 1, 3):
            part_copy(axis, d, y if axis else x).start()

    def part_finish(axis):
        for d in range(1, SIDE):
            part_copy(axis, d, y if axis else x).wait_send()

    def part_total(axis):
        for d in (1, 3, 2):
            part_copy(axis, d, wrap((y if axis else x) - d, SIDE)).wait_recv()
        slots = [part_buf[axis * SIDE + i] for i in range(SIDE)]
        return (slots[0] + slots[1]) + (slots[2] + slots[3])

    sum_start, sum_arrive, sum_finish = share(sum_buf, sum_send, sum_recv, False)
    tot_start, tot_arrive, tot_finish = share(tot_buf, tot_send, tot_recv, True)

    def over(i, other):
        slot = wrap(z + i, DEPTH) * 2 + (1 - core if other else core)
        return pltpu.make_async_remote_copy(
            src_ref=sum_buf.at[slot], dst_ref=sum_buf.at[slot], send_sem=over_send.at[i], recv_sem=over_recv.at[i],
            device_id=partner, device_id_type=MESH,
        )

    def over_all(act):
        def one(i, carry):
            act(i)
            return carry

        lax.fori_loop(0, DEPTH, one, 0)

    pl.semaphore_wait(barrier, lower)
    for number, (neighbour, theirs, mine) in enumerate(links):

        @pl.when(theirs < mine)
        def _(neighbour=neighbour, number=number):
            pl.semaphore_signal(ready_sem.at[number ^ 1], inc=1, device_id=neighbour, device_id_type=MESH)

    acc[...] = jnp.zeros_like(acc)
    for load in loads[:2]:
        load.wait()
    for j in range(TILES):
        cols = slice(j * TB, (j + 1) * TB)
        part = jnp.zeros((1, TB), jnp.float32)
        for i in range(TILES):
            rows = slice(i * TB, (i + 1) * TB)
            tile = own[rows, cols].astype(jnp.float32) * tile_ref[i, j].astype(jnp.float32)
            part += jnp.sum(tile, axis=0, keepdims=True)
            rows_buf[me_col, AUG + i * TB : AUG + (i + 1) * TB, cols] = tile.astype(jnp.bfloat16)
            cols_buf[me_row, rows, cols] = tile.astype(jnp.bfloat16)
        part_buf[x, :, cols] = part

    for load in loads[2:]:
        load.wait()

    def early(number):
        _, theirs, mine = links[number]

        @pl.when(theirs < mine)
        def _():
            send(0, number, (2,) if number < 4 else None)

    def late(number):
        _, theirs, mine = links[number]

        @pl.when(theirs > mine)
        def _():
            pl.semaphore_wait(ready_sem.at[number], 1)
            send(0, number, (2,) if number < 4 else None)

    for number in range(6):
        early(number)
    for number in range(5):
        late(number)
    spread_plane(0)
    part_start(0)
    for number in range(4):
        send(0, number, (4,))
    late(5)
    send(0)
    spread_depth(0)

    def multiply(low, high):
        def one(k, carry):
            dx = wrap(lax.div(k, SIDE) - x, SIDE)
            dy = wrap(lax.rem(k, SIDE) - y, SIDE)
            dz = wrap(lax.div(k, 2) - z, DEPTH)

            def far(d):
                return lax.div(d * (SIDE - d), 4)

            def off(d):
                return lax.div(d + 3, 4)

            n, both = far(dx) + far(dy), off(dx) * off(dy)
            slow = lax.rem(k + core, 2)
            by_plane = n * (2 - n) * (1 - both + both * lax.div(11 - dx - dy, 2)) + 6 * lax.div(n * (n - 1), 2)
            reach = dz * (DEPTH - dz)
            by_depth = lax.div(reach, 15) * (2 + 2 * slow) + 3 * lax.div(reach, 16)

            ready = jnp.maximum(by_plane, by_depth)

            @pl.when((ready >= low) & (ready <= high))
            def _():
                acc[...] += jnp.dot(rows_buf[k], cols_buf[k], preferred_element_type=jnp.float32)

            return carry

        lax.fori_loop(0, GROUP, one, 0)

    for event in sorted({arrives for _, arrives, *_ in copies}):
        receive(event)
        if event == 2:
            part_buf[SIDE + y] = part_total(0)
            part_finish(0)
            part_start(1)
        send(event)
        if event == 2:
            spread_depth(1)
        if event == 2.1:
            spread_depth(2)
        if event == 4:
            spread_plane(1)
        if event == 5:
            sum_buf[me_col] = part_total(1)
            part_finish(1)
            sum_start()
        if event == 7:
            spread_plane(2)
        if event == 9:
            sum_arrive()
            over_all(lambda i: over(i, 0).start())
        if event == 10.1:
            over_all(lambda i: over(i, 1).wait_recv())

            def augment(k, carry):
                s = sum_buf[k]
                high = s.astype(jnp.bfloat16).astype(jnp.float32)
                rest = s - high
                mid = rest.astype(jnp.bfloat16).astype(jnp.float32)
                low = rest - mid
                index = lax.broadcasted_iota(jnp.int32, (AUG, BLOCK), 0)
                rows = jnp.where(index == 0, high, jnp.where(index == 1, mid, jnp.where(index == 2, low, 0.0)))
                rows_buf[k, :AUG, :] = rows.astype(jnp.bfloat16)
                return carry

            lax.fori_loop(0, GROUP, augment, 0)
        if event in (10.1, 12):
            pl.when(z > 0 if event == 10.1 else z == 0)(functools.partial(multiply, 0, 1))
        if event in STAGE_AFTER:
            multiply(*STAGE_AFTER[event])

    def product(k):
        return jnp.dot(rows_buf[k], cols_buf[k], preferred_element_type=jnp.float32)

    def finish(last):
        total = acc[...] + last
        means = (total[0:1] + total[1:2] + total[2:3]) / ORDER
        cut = 0.125 * thr_ref[...].astype(jnp.float32) * means
        for j in range(TILES):
            cols = slice(j * TB, (j + 1) * TB)
            part = jnp.zeros((1, TB), jnp.float32)
            for i in range(TILES):
                tile = total[AUG + i * TB : AUG + (i + 1) * TB, cols]
                tile = jnp.maximum(tile - cut[:, cols], 0.0) * keep_ref[i, j].astype(jnp.float32)
                pruned_ref[i * TB : (i + 1) * TB, cols] = tile
                part += jnp.sum(tile, axis=0, keepdims=True)
            tot_buf[me_row, :, cols] = part

    far_col, far_row = row_of(2, 2), col_of(4, 1)

    @pl.when(far_col != far_row)
    def _():
        acc[...] += product(far_col) + product(far_row)

    @pl.when(far_col == far_row)
    def _():
        acc[...] += product(far_col)

    finish(0.0)

    sum_finish()
    tot_start()
    for _, _, _, out, _ in copies:
        out.wait_send()
    over_all(lambda i: over(i, 0).wait_send())

    @pl.when(z < DEPTH - 1)
    def _():
        seam_up.wait_send()

    @pl.when(z == 1)
    def _():
        seam_down.wait_send()

    tot_arrive()
    totals = tot_buf[0]
    for i in range(1, GROUP):
        totals += tot_buf[i]
    scale_ref[...] = jnp.maximum(totals / ORDER, 0.1)
    tot_finish()


def n_copies():
    return 40 + 16 + 18 + 2


def on_device(values, tile_mask, keep_mask, thr_index):
    vmem = pl.BlockSpec(memory_space=pltpu.VMEM)
    hbm = pl.BlockSpec(memory_space=pltpu.HBM)
    dma = pltpu.SemaphoreType.DMA
    pruned, scale = pl.pallas_call(
        kernel,
        out_shape=(
            jax.ShapeDtypeStruct((BLOCK, BLOCK), jnp.float32),
            jax.ShapeDtypeStruct((1, BLOCK), jnp.float32),
        ),
        in_specs=[hbm, hbm, hbm, hbm],
        out_specs=(vmem, vmem),
        scratch_shapes=[
            pltpu.SMEM((TILES, TILES), jnp.int32),
            pltpu.SMEM((TILES, TILES), jnp.int32),
            pltpu.VMEM((1, BLOCK), jnp.int32),
            pltpu.VMEM((GROUP, BLOCK + AUG, BLOCK), jnp.bfloat16),
            pltpu.VMEM((GROUP, BLOCK, BLOCK), jnp.bfloat16),
            pltpu.VMEM((BLOCK + AUG, BLOCK), jnp.float32),
            pltpu.VMEM((BLOCK, BLOCK), jnp.bfloat16),
            pltpu.VMEM((2 * SIDE, 1, BLOCK), jnp.float32),
            pltpu.VMEM((GROUP, 1, BLOCK), jnp.float32),
            pltpu.VMEM((GROUP, 1, BLOCK), jnp.float32),
            dma((4,)), dma((n_copies(),)), dma((n_copies(),)),
            dma((2 * SIDE,)), dma((2 * SIDE,)), dma((DEPTH,)), dma((DEPTH,)), dma((GROUP,)), dma((GROUP,)),
            dma((DEPTH,)), dma((DEPTH,)),
            pltpu.SemaphoreType.REGULAR((6,)), pltpu.SemaphoreType.REGULAR((ROUNDS,)), pltpu.SemaphoreType.REGULAR((ROUNDS,)),
        ],
        compiler_params=pltpu.CompilerParams(
            collective_id=0, has_side_effects=True, vmem_limit_bytes=40 * 1024 * 1024
        ),
        cost_estimate=pl.CostEstimate(
            flops=2 * BLOCK * BLOCK * ORDER, bytes_accessed=2 * 1024 * 1024, transcendentals=0
        ),
        name="expand",
    )(*(pltpu.with_memory_space_constraint(a, pltpu.HBM) for a in (values, tile_mask, keep_mask, thr_index.reshape(1, BLOCK))))
    return (pruned / scale).astype(jnp.bfloat16)


def solution(mesh):
    return jax.shard_map(
        on_device,
        mesh=mesh,
        in_specs=(P("row", "col"), P("row", "col"), P("row", "col"), P("col")),
        out_specs=P("row", "col"),
        check_vma=False,
    )
```

```python
import functools

import jax
import jax.numpy as jnp
from jax import lax
from jax.experimental import pallas as pl
from jax.experimental.pallas import tpu as pltpu
from jax.sharding import PartitionSpec as P

TB = 128
BLOCK = 512
HALF = BLOCK // 2
QUART = BLOCK // 4
TILES = BLOCK // TB
GROUP = 16
SIDE = 4
DEPTH = 8
ORDER = BLOCK * GROUP
AUG = 16
ROUNDS = 3
MESH = pl.DeviceIdType.MESH

UPPER, LOWER = (0, HALF), (HALF, HALF)


def quarter(half, step):
    return (half[0] + (0 if step > 0 else QUART), QUART)


def plane_queue(axis, step):
    def at(along, across):
        return (along, across) if axis == 0 else (across, along)

    first, second = (UPPER, LOWER) if axis == 0 else (LOWER, UPPER)
    return [
        (at(0, 0), first, 0, 2),
        (at(0, 0), second, 0, 4),
        (at(-step, 0), quarter(first, step), 2, 5),
        (at(0, -1), second, 2, 7),
        (at(0, 1), second, 2, 9),
        (at(-step, 0), quarter(second, step), 4, 10),
        (at(0, 2), second, 5, 12),
        (at(-step, -1), quarter(second, step), 7, 13),
        (at(-step, 1), quarter(second, step), 9, 14),
        (at(-step, 2), quarter(second, step), 12, 15),
    ]


SEAM = (192, 64)


def depth_queue(step):
    first, second = (UPPER, LOWER) if step > 0 else (LOWER, UPPER)
    last = ((0, 128), (128, 64)) if step > 0 else ((256, 128), (384, 128))
    return [
        (0, first, 0, 2.1),
        (0, second, 0, 4.1),
        (-step, first, 2.1, 6.1),
        (-step, second, 4.1, 8.1),
        (-2 * step, first, 6.1, 10.1),
        (-2 * step, second, 8.1, 12.1),
        (-3 * step, last[0], 10.1, 13.1 if step > 0 else 13.08),
        (-3 * step, last[1], 10.1, 14.1 if step > 0 else 14.08),
    ]


def chip_queue():
    moves = [(0, UPPER, 0, 9.2), (0, LOWER, 0, 9.2)]
    for step in (1, -1):
        first, second = (UPPER, LOWER) if step > 0 else (LOWER, UPPER)
        moves += [
            (-step, first, 2.1, 9.2),
            (-step, second, 4.1, 9.2),
            (-2 * step, first, 6.1, 9.2),
            (-2 * step, second, 8.1, 9.2),
            (-3 * step, first, 10.1, 14.2),
            (-3 * step, second, 12.1, 14.2),
            (-4 * step, quarter(first, 1), 13.1 if step > 0 else 13.08, 15.2),
            (-4 * step, quarter(first, -1), 14.1 if step > 0 else 14.08, 15.2),
        ]
    return sorted(moves, key=lambda move: move[2])


STAGE_AFTER = {12.1: (2, 2), 13: (3, 3), 14.2: (4, 5)}


def wrap(value, size):
    return lax.rem(value + size, size)


def kernel(
    values_ref, tile_hbm, keep_hbm, thr_hbm, pruned_ref, scale_ref, tile_ref, keep_ref, thr_ref,
    rows_buf, cols_buf, acc, own, part_buf, sum_buf, tot_buf,
    in_sem, send_sem, recv_sem, part_send, part_recv, sum_send, sum_recv, tot_send, tot_recv, over_send, over_recv,
    ready_sem, plane_sem, depth_sem,
):
    me_row, me_col = lax.axis_index("row"), lax.axis_index("col")
    x, y = lax.div(me_row, SIDE), lax.rem(me_row, SIDE)
    z, core = lax.div(me_col, 2), lax.rem(me_col, 2)

    def row_of(dx, dy):
        return wrap(x + dx, SIDE) * SIDE + wrap(y + dy, SIDE)

    def col_of(dz, other=0):
        return wrap(z + dz, DEPTH) * 2 + (1 - core if other else core)

    loads = [
        pltpu.make_async_copy(out, into, in_sem.at[i])
        for i, (out, into) in enumerate(
            ((values_ref, own), (tile_hbm, tile_ref), (keep_hbm, keep_ref), (thr_hbm, thr_ref))
        )
    ]
    for load in loads:
        load.start()

    links = []
    for axis in (0, 1):
        for step in (1, -1):
            dx, dy = (step, 0) if axis == 0 else (0, step)
            mine = x if axis == 0 else y
            links.append(((row_of(dx, dy), me_col), wrap(mine + step, SIDE), mine))
    for step in (1, -1):
        links.append(((me_row, col_of(step)), wrap(z + step, DEPTH), z))
    partner = (me_row, col_of(0, 1))

    barrier = pltpu.get_barrier_semaphore()
    pl.semaphore_signal(barrier, inc=1, device_id=partner, device_id_type=MESH)
    lower = 1
    for neighbour, theirs, mine in links:
        lower += (theirs < mine).astype(jnp.int32)

        @pl.when(theirs > mine)
        def _(neighbour=neighbour):
            pl.semaphore_signal(barrier, inc=1, device_id=neighbour, device_id_type=MESH)

    copies = []

    def copy_of(buf, slot, rows, number, target):
        above = AUG if buf is rows_buf else 0
        part = buf.at[slot, pl.ds(rows[0] + above, rows[1]), :]
        return pltpu.make_async_remote_copy(
            src_ref=part, dst_ref=part, send_sem=send_sem.at[number], recv_sem=recv_sem.at[number],
            device_id=target, device_id_type=MESH,
        )

    def add(buf, sent_slot, got_slot, rows, target, leaves, arrives, link=None):
        number = len(copies)
        copies.append((
            leaves, arrives, link,
            copy_of(buf, sent_slot, rows, number, target),
            copy_of(buf, got_slot, rows, number, target),
        ))

    for place in range(10):
        for axis in (0, 1):
            for step in (1, -1):
                (dx, dy), rows, leaves, arrives = plane_queue(axis, step)[place]
                sx, sy = (step, 0) if axis == 0 else (0, step)
                add(
                    cols_buf, row_of(dx, dy), row_of(dx - sx, dy - sy), rows,
                    (row_of(sx, sy), me_col), leaves, arrives, 2 * axis + (step < 0),
                )
        if place < 8:
            for step in (1, -1):
                dz, rows, leaves, arrives = depth_queue(step)[place]
                add(
                    rows_buf, col_of(dz), col_of(dz - step), rows,
                    (me_row, col_of(step)), leaves, arrives, 4 + (step < 0),
                )
    for dz, rows, leaves, arrives in chip_queue():
        add(rows_buf, col_of(dz), col_of(dz, 1), rows, partner, leaves, arrives)

    seam = len(copies)
    seam_up = copy_of(rows_buf, col_of(-3), SEAM, seam, (me_row, col_of(1)))
    seam_in = copy_of(rows_buf, col_of(4), SEAM, seam, (me_row, col_of(1)))
    part = rows_buf.at[col_of(3), pl.ds(SEAM[0] + AUG, SEAM[1]), :]
    seam_down = pltpu.make_async_remote_copy(
        src_ref=part, dst_ref=part, send_sem=send_sem.at[seam + 1], recv_sem=recv_sem.at[seam],
        device_id=(me_row, col_of(-1)), device_id_type=MESH,
    )

    def send(event, link=None, places=None):
        for leaves, arrives, on, out, _ in copies:
            if leaves == event and (event > 0 or on == link) and (places is None or arrives in places):
                out.start()
        if event == 10.1:

            @pl.when(z < DEPTH - 1)
            def _():
                seam_up.start()

        if event == 12.1:

            @pl.when(z == 1)
            def _():
                seam_down.start()

    def receive(event):
        for _, arrives, _, _, into in copies:
            if arrives == event:
                into.wait_recv()
        if event == 14.1:
            seam_in.wait_recv()

    def spread(sem, number, neighbours):
        for neighbour in neighbours:
            pl.semaphore_signal(sem.at[number], inc=1, device_id=neighbour, device_id_type=MESH)
        pl.semaphore_wait(sem.at[number], len(neighbours))

    def spread_plane(number):
        spread(plane_sem, number, [link[0] for link in links[:4]])

    def spread_depth(number):
        spread(depth_sem, number, [link[0] for link in links[4:]])

    def share(buf, sends, recvs, along_row):
        count = GROUP if along_row else DEPTH

        def slot_of(i):
            return lax.rem(me_row + i, GROUP) if along_row else wrap(z + i, DEPTH) * 2 + core

        def copy(i, slot):
            target = (slot_of(i), me_col) if along_row else (me_row, slot_of(i))
            return pltpu.make_async_remote_copy(
                src_ref=buf.at[slot], dst_ref=buf.at[slot], send_sem=sends.at[i], recv_sem=recvs.at[i],
                device_id=target, device_id_type=MESH,
            )

        def start(i, carry):
            copy(i, slot_of(0)).start()
            return carry

        def arrive(i, carry):
            copy(i, slot_of(count - i)).wait_recv()
            return carry

        def finish(i, carry):
            copy(i, slot_of(0)).wait_send()
            return carry

        return tuple(functools.partial(lax.fori_loop, 1, count, f, 0) for f in (start, arrive, finish))


    def part_copy(axis, d, slot):
        number = axis * SIDE + d
        return pltpu.make_async_remote_copy(
            src_ref=part_buf.at[axis * SIDE + slot], dst_ref=part_buf.at[axis * SIDE + slot],
            send_sem=part_send.at[number], recv_sem=part_recv.at[number],
            device_id=(row_of(0, d) if axis else row_of(d, 0), me_col), device_id_type=MESH,
        )

    def part_start(axis):
        for d in (2, 1, 3):
            part_copy(axis, d, y if axis else x).start()

    def part_finish(axis):
        for d in range(1, SIDE):
            part_copy(axis, d, y if axis else x).wait_send()

    def part_total(axis):
        for d in (1, 3, 2):
            part_copy(axis, d, wrap((y if axis else x) - d, SIDE)).wait_recv()
        slots = [part_buf[axis * SIDE + i] for i in range(SIDE)]
        return (slots[0] + slots[1]) + (slots[2] + slots[3])

    sum_start, sum_arrive, sum_finish = share(sum_buf, sum_send, sum_recv, False)

    def total_copy(dx, dy, slot):
        return pltpu.make_async_remote_copy(
            src_ref=tot_buf.at[slot], dst_ref=tot_buf.at[slot],
            send_sem=tot_send.at[dx * SIDE + dy], recv_sem=tot_recv.at[dx * SIDE + dy],
            device_id=(row_of(dx, dy), me_col), device_id_type=MESH,
        )

    apart = sorted(
        ((dx, dy) for dx in range(SIDE) for dy in range(SIDE) if dx or dy),
        key=lambda d: -sum(min(v, SIDE - v) for v in d),
    )

    def over(i, other):
        slot = wrap(z + i, DEPTH) * 2 + (1 - core if other else core)
        return pltpu.make_async_remote_copy(
            src_ref=sum_buf.at[slot], dst_ref=sum_buf.at[slot], send_sem=over_send.at[i], recv_sem=over_recv.at[i],
            device_id=partner, device_id_type=MESH,
        )

    def over_all(act):
        def one(i, carry):
            act(i)
            return carry

        lax.fori_loop(0, DEPTH, one, 0)

    pl.semaphore_wait(barrier, lower)
    for number, (neighbour, theirs, mine) in enumerate(links):

        @pl.when(theirs < mine)
        def _(neighbour=neighbour, number=number):
            pl.semaphore_signal(ready_sem.at[number ^ 1], inc=1, device_id=neighbour, device_id_type=MESH)

    acc[...] = jnp.zeros_like(acc)
    for load in loads[:2]:
        load.wait()
    for j in range(TILES):
        cols = slice(j * TB, (j + 1) * TB)
        part = jnp.zeros((1, TB), jnp.float32)
        for i in range(TILES):
            rows = slice(i * TB, (i + 1) * TB)
            tile = own[rows, cols].astype(jnp.float32) * tile_ref[i, j].astype(jnp.float32)
            part += jnp.sum(tile, axis=0, keepdims=True)
            rows_buf[me_col, AUG + i * TB : AUG + (i + 1) * TB, cols] = tile.astype(jnp.bfloat16)
            cols_buf[me_row, rows, cols] = tile.astype(jnp.bfloat16)
        part_buf[x, :, cols] = part

    for load in loads[2:]:
        load.wait()

    def early(number):
        _, theirs, mine = links[number]

        @pl.when(theirs < mine)
        def _():
            send(0, number, (2,) if number < 4 else None)

    def late(number):
        _, theirs, mine = links[number]

        @pl.when(theirs > mine)
        def _():
            pl.semaphore_wait(ready_sem.at[number], 1)
            send(0, number, (2,) if number < 4 else None)

    for number in (4, 5, 0, 1, 2, 3):
        early(number)
    send(0)
    for number in range(5):
        late(number)
    spread_plane(0)
    part_start(0)
    for number in range(4):
        send(0, number, (4,))
    late(5)
    spread_depth(0)

    def multiply(low, high):
        def one(k, carry):
            dx = wrap(lax.div(k, SIDE) - x, SIDE)
            dy = wrap(lax.rem(k, SIDE) - y, SIDE)
            dz = wrap(lax.div(k, 2) - z, DEPTH)

            def far(d):
                return lax.div(d * (SIDE - d), 4)

            def off(d):
                return lax.div(d + 3, 4)

            n, both = far(dx) + far(dy), off(dx) * off(dy)
            slow = lax.rem(k + core, 2)
            by_plane = n * (2 - n) * (1 - both + both * lax.div(11 - dx - dy, 2)) + 6 * lax.div(n * (n - 1), 2)
            reach = dz * (DEPTH - dz)
            by_depth = lax.div(reach, 15) * (2 + 2 * slow) + 3 * lax.div(reach, 16)

            ready = jnp.maximum(by_plane, by_depth)

            @pl.when((ready >= low) & (ready <= high))
            def _():
                acc[...] += jnp.dot(rows_buf[k], cols_buf[k], preferred_element_type=jnp.float32)

            return carry

        lax.fori_loop(0, GROUP, one, 0)

    for event in sorted({arrives for _, arrives, *_ in copies}):
        receive(event)
        if event == 2:
            part_buf[SIDE + y] = part_total(0)
            part_finish(0)
            part_start(1)
        send(event)
        if event == 2:
            spread_depth(1)
        if event == 2.1:
            spread_depth(2)
        if event == 4:
            spread_plane(1)
        if event == 5:
            sum_buf[me_col] = part_total(1)
            part_finish(1)
            sum_start()
        if event == 7:
            spread_plane(2)
        if event == 9:
            sum_arrive()
            over_all(lambda i: over(i, 0).start())
        if event == 10.1:
            over_all(lambda i: over(i, 1).wait_recv())

            def augment(k, carry):
                s = sum_buf[k]
                high = s.astype(jnp.bfloat16).astype(jnp.float32)
                rest = s - high
                mid = rest.astype(jnp.bfloat16).astype(jnp.float32)
                low = rest - mid
                index = lax.broadcasted_iota(jnp.int32, (AUG, BLOCK), 0)
                rows = jnp.where(index == 0, high, jnp.where(index == 1, mid, jnp.where(index == 2, low, 0.0)))
                rows_buf[k, :AUG, :] = rows.astype(jnp.bfloat16)
                return carry

            lax.fori_loop(0, GROUP, augment, 0)
        if event in (10.1, 12):
            pl.when(z > 0 if event == 10.1 else z == 0)(functools.partial(multiply, 0, 1))
        if event in STAGE_AFTER:
            multiply(*STAGE_AFTER[event])

    def product(k):
        return jnp.dot(rows_buf[k], cols_buf[k], preferred_element_type=jnp.float32)

    def finish(last):
        total = acc[...] + last
        means = (total[0:1] + total[1:2] + total[2:3]) / ORDER
        cut = 0.125 * thr_ref[...].astype(jnp.float32) * means
        for j in range(TILES):
            cols = slice(j * TB, (j + 1) * TB)
            part = jnp.zeros((1, TB), jnp.float32)
            for i in range(TILES):
                tile = total[AUG + i * TB : AUG + (i + 1) * TB, cols]
                tile = jnp.maximum(tile - cut[:, cols], 0.0) * keep_ref[i, j].astype(jnp.float32)
                pruned_ref[i * TB : (i + 1) * TB, cols] = tile
                part += jnp.sum(tile, axis=0, keepdims=True)
            tot_buf[me_row, :, cols] = part

    far_col, far_row = row_of(2, 2), col_of(4, 1)

    @pl.when(far_col != far_row)
    def _():
        acc[...] += product(far_col) + product(far_row)

    @pl.when(far_col == far_row)
    def _():
        acc[...] += product(far_col)

    finish(0.0)

    sum_finish()
    for dx, dy in apart:
        total_copy(dx, dy, me_row).start()
    for _, _, _, out, _ in copies:
        out.wait_send()
    over_all(lambda i: over(i, 0).wait_send())

    @pl.when(z < DEPTH - 1)
    def _():
        seam_up.wait_send()

    @pl.when(z == 1)
    def _():
        seam_down.wait_send()

    for dx, dy in apart:
        total_copy(dx, dy, row_of(-dx, -dy)).wait_recv()
    totals = tot_buf[0]
    for i in range(1, GROUP):
        totals += tot_buf[i]
    scale_ref[...] = jnp.maximum(totals / ORDER, 0.1)
    for dx, dy in apart:
        total_copy(dx, dy, me_row).wait_send()


def n_copies():
    return 40 + 16 + 18 + 2


def on_device(values, tile_mask, keep_mask, thr_index):
    vmem = pl.BlockSpec(memory_space=pltpu.VMEM)
    hbm = pl.BlockSpec(memory_space=pltpu.HBM)
    dma = pltpu.SemaphoreType.DMA
    pruned, scale = pl.pallas_call(
        kernel,
        out_shape=(
            jax.ShapeDtypeStruct((BLOCK, BLOCK), jnp.float32),
            jax.ShapeDtypeStruct((1, BLOCK), jnp.float32),
        ),
        in_specs=[hbm, hbm, hbm, hbm],
        out_specs=(vmem, vmem),
        scratch_shapes=[
            pltpu.SMEM((TILES, TILES), jnp.int32),
            pltpu.SMEM((TILES, TILES), jnp.int32),
            pltpu.VMEM((1, BLOCK), jnp.int32),
            pltpu.VMEM((GROUP, BLOCK + AUG, BLOCK), jnp.bfloat16),
            pltpu.VMEM((GROUP, BLOCK, BLOCK), jnp.bfloat16),
            pltpu.VMEM((BLOCK + AUG, BLOCK), jnp.float32),
            pltpu.VMEM((BLOCK, BLOCK), jnp.bfloat16),
            pltpu.VMEM((2 * SIDE, 1, BLOCK), jnp.float32),
            pltpu.VMEM((GROUP, 1, BLOCK), jnp.float32),
            pltpu.VMEM((GROUP, 1, BLOCK), jnp.float32),
            dma((4,)), dma((n_copies(),)), dma((n_copies(),)),
            dma((2 * SIDE,)), dma((2 * SIDE,)), dma((DEPTH,)), dma((DEPTH,)), dma((GROUP,)), dma((GROUP,)),
            dma((DEPTH,)), dma((DEPTH,)),
            pltpu.SemaphoreType.REGULAR((6,)), pltpu.SemaphoreType.REGULAR((ROUNDS,)), pltpu.SemaphoreType.REGULAR((ROUNDS,)),
        ],
        compiler_params=pltpu.CompilerParams(
            collective_id=0, has_side_effects=True, vmem_limit_bytes=40 * 1024 * 1024
        ),
        cost_estimate=pl.CostEstimate(
            flops=2 * BLOCK * BLOCK * ORDER, bytes_accessed=2 * 1024 * 1024, transcendentals=0
        ),
        name="expand",
    )(*(pltpu.with_memory_space_constraint(a, pltpu.HBM) for a in (values, tile_mask, keep_mask, thr_index.reshape(1, BLOCK))))
    return (pruned / scale).astype(jnp.bfloat16)


def solution(mesh):
    return jax.shard_map(
        on_device,
        mesh=mesh,
        in_specs=(P("row", "col"), P("row", "col"), P("row", "col"), P("col")),
        out_specs=P("row", "col"),
        check_vma=False,
    )
```
